16 devices in a mesh: rep: 4 (over y, z, core), dp: 4 (over x).
Axes of the slice: x: 4, y: 2, z: 1, core: 2. Of those that a mesh axis runs over, the one named last changes fastest.
The devices are a block of a 4x4x8 slice.
Arguments:
- x: bfloat16 [16, 4096, 1024], P(('rep', 'dp')), parts along dimension 0
- dy: bfloat16 [16, 4096, 1024], P(('rep', 'dp')), parts along dimension 0
- w_gate: bfloat16 [2, 1024, 3200], replicated
- w_up: bfloat16 [2, 1024, 3200], replicated
- w_down: bfloat16 [2, 3200, 1024], replicated
- m_w_gate: float32 [2, 1024, 3200], P(None, 'dp')
- m_w_up: float32 [2, 1024, 3200], P(None, 'dp')
- m_w_down: float32 [2, 3200, 1024], P(None, 'dp')
- v_w_gate: float32 [2, 1024, 3200], P(None, 'dp')
- v_w_up: float32 [2, 1024, 3200], P(None, 'dp')
- v_w_down: float32 [2, 3200, 1024], P(None, 'dp')
Outputs:
- output 1: bfloat16 [8, 1024, 3200], P('rep'), parts along dimension 0
- output 2: bfloat16 [8, 1024, 3200], P('rep'), parts along dimension 0
- output 3: bfloat16 [8, 3200, 1024], P('rep'), parts along dimension 0
- output 4: float32 [8, 1024, 3200], P('rep', 'dp'), parts along dimension 0
- output 5: float32 [8, 1024, 3200], P('rep', 'dp'), parts along dimension 0
- output 6: float32 [8, 3200, 1024], P('rep', 'dp'), parts along dimension 0
- output 7: float32 [8, 1024, 3200], P('rep', 'dp'), parts along dimension 0
- output 8: float32 [8, 1024, 3200], P('rep', 'dp'), parts along dimension 0
- output 9: float32 [8, 3200, 1024], P('rep', 'dp'), parts along dimension 0
There are 4 independent parts. The reference program is written for one: setup_inputs(seed, part) draws one part's arguments, and reference() takes and returns one part's arrays. A program takes and returns all parts, laid end to end along the dimension named above; an argument that names none is the same for every part.
All inputs are finite; a program needn't handle non-finite values.
Results may differ from the reference program's by a relative error of at most 0.022.
Values are sent between devices in bfloat16 or wider.
A program may use at most 768 MiB of HBM per device.

```python
import jax
import jax.numpy as jnp
from jax import lax

SEQUENCES = 4
TOKENS = 4096
D = 1024
FF = 3200
LAYERS = 2
NAMES = ("w_gate", "w_up", "w_down")
SHAPES = {"w_gate": (LAYERS, D, FF), "w_up": (LAYERS, D, FF), "w_down": (LAYERS, FF, D)}


def bump(key, n, height):
    away = (jnp.arange(n, dtype=jnp.int32) - jax.random.randint(key, (), 0, n, jnp.int32)) % n
    return jnp.where(away < n // 8, height, 1.0)


def together(key, own, strength):
    shared = jax.random.normal(key, own.shape[1:], jnp.float32)
    return (own + strength * shared) * lax.rsqrt(1 + strength * strength)


def setup_inputs(seed: int = 0, part: int = 0) -> dict:
    kx, kdy, ka, kb, kz, kf, kh, kl, *keys = jax.random.split(jax.random.key(seed), 8 + 3 * len(NAMES))
    kx, kdy, ka, kb = (jax.random.fold_in(k, part) for k in (kx, kdy, ka, kb))
    kw, km, kv = (keys[i::3] for i in range(3))
    shape = (SEQUENCES, TOKENS, D)
    much_x, much_dy = jax.random.uniform(kz, (2,), jnp.float32, 0.0, 1.0)
    loud = 2.0 ** jax.random.uniform(jax.random.fold_in(kz, 1), (), jnp.float32, -1.0, 2.0)
    layers = 2.0 ** jax.random.uniform(kl, (LAYERS, 1, 1), jnp.float32, -1.0, 1.0)
    x = together(ka, jax.random.normal(kx, shape, jnp.float32), much_x) * bump(kf, D, 4.0)
    dy = together(kb, jax.random.normal(kdy, shape, jnp.float32), much_dy)
    drawn = {"x": x.astype(jnp.bfloat16), "dy": (loud * dy * (SEQUENCES * TOKENS) ** -0.5).astype(jnp.bfloat16)}
    for key, name in zip(kw, NAMES, strict=True):
        w = jax.random.normal(key, SHAPES[name], jnp.float32) * SHAPES[name][1] ** -0.5
        drawn[name] = (w * {"w_gate": 1.0, "w_up": bump(kh, FF, 4.0), "w_down": layers}[name]).astype(jnp.bfloat16)
    for key, name in zip(km, NAMES, strict=True):
        drawn[f"m_{name}"] = 0.1 * jax.random.normal(key, SHAPES[name], jnp.float32)
    for key, name in zip(kv, NAMES, strict=True):
        drawn[f"v_{name}"] = jax.random.uniform(key, SHAPES[name], jnp.float32, 0.005, 0.015)
    return drawn


def matmul(a, w):
    return jnp.dot(a, w, preferred_element_type=jnp.float32).astype(jnp.bfloat16)


def normed(h):
    wide = h.astype(jnp.float32)
    scale = lax.rsqrt(jnp.mean(wide**2, -1, keepdims=True) + 1e-6)
    return (wide * scale).astype(jnp.bfloat16)


def layer(h, w):
    a = normed(h)
    gate = jnp.dot(a, w["w_gate"], preferred_element_type=jnp.float32)
    up = jnp.dot(a, w["w_up"], preferred_element_type=jnp.float32)
    return h + matmul((jax.nn.silu(gate) * up).astype(jnp.bfloat16), w["w_down"])


def adamw(w, m, v, g):
    m = 0.9 * m + 0.1 * g
    v = 0.95 * v + 0.05 * g * g
    step = m * lax.rsqrt(v + 1e-8) + 0.1 * w
    return (w - 0.02 * step).astype(jnp.bfloat16), m, v


def clipped(gradients, sum_of_squares, count):
    factor = jnp.minimum(1.0, 0.5 * lax.rsqrt(sum_of_squares / count + 1e-30))
    return [g * factor for g in gradients]


def stack(weights, h):
    return lax.scan(lambda h, w: (layer(h, w), None), h, weights)[0]


def reference(x, dy, w_gate, w_up, w_down, m_w_gate, m_w_up, m_w_down, v_w_gate, v_w_up, v_w_down):
    weights = dict(zip(NAMES, (w_gate, w_up, w_down), strict=True))

    def take(so_far, sequence):
        h, by_y = sequence
        _, back = jax.vjp(lambda w: stack(w, h), weights)
        return jax.tree.map(lambda total, term: total + term.astype(jnp.float32), so_far, back(by_y)[0]), None

    none_yet = {name: jnp.zeros(w.shape, jnp.float32) for name, w in weights.items()}
    by_weights, _ = lax.scan(take, none_yet, (x, dy))
    gradients = [by_weights[name].astype(jnp.bfloat16).astype(jnp.float32) for name in NAMES]
    gradients = clipped(gradients, sum(jnp.sum(g * g) for g in gradients), sum(g.size for g in gradients))
    new = [
        adamw(w.astype(jnp.float32), m, v, g)
        for w, m, v, g in zip((w_gate, w_up, w_down), (m_w_gate, m_w_up, m_w_down), (v_w_gate, v_w_up, v_w_down), gradients, strict=True)
    ]
    return tuple(one[which] for which in range(3) for one in new)
```

```python
import functools
import jax, jax.numpy as jnp
from jax import lax
from jax.experimental import pallas as pl
from jax.experimental.pallas import tpu as pltpu
from jax.sharding import PartitionSpec as P

F32, BF16 = jnp.float32, jnp.bfloat16
def dot(a, b): return jnp.dot(a, b, preferred_element_type=F32)
def dot_nt(a, b): return lax.dot_general(a, b, (((1,), (1,)), ((), ())), preferred_element_type=F32)
def sigmoid(x): return 0.5 * jnp.tanh(0.5 * x) + 0.5

def fwd_kernel(chunk, with_down, h_ref, wg_ref, wu_ref, *refs):
    if with_down: wd_ref, aT_ref, gate_ref, up_ref, actT_ref, h1_ref, a_ref, act_ref, wt_ref = refs
    else: aT_ref, gate_ref, up_ref, actT_ref, a_ref, wt_ref = refs
    ff = wg_ref.shape[1]; full = ff // chunk; tail = ff - full * chunk
    @pl.when(pl.program_id(0) == 0)
    def _():
        wt_ref[:, :tail] = wg_ref[:, full*chunk:]; wt_ref[:, tail:] = wu_ref[:, full*chunk:]
    wide = h_ref[...].astype(F32)
    scale = lax.rsqrt(jnp.mean(wide * wide, -1, keepdims=True) + 1e-6)
    a = (wide * scale).astype(BF16)
    a_ref[...] = a
    aT_ref[...] = a.T
    def part(g, u, cols):
        gate_ref[:, cols] = g; up_ref[:, cols] = u
        act = (g * sigmoid(g) * u).astype(BF16)
        if with_down: act_ref[:, cols] = act
        actT_ref[cols, :] = act.T
    for c in range(full):
        cols = pl.ds(c * chunk, chunk)
        part(dot(a_ref[...], wg_ref[:, cols]), dot(a_ref[...], wu_ref[:, cols]), cols)
    gu = dot(a_ref[...], wt_ref[...])
    part(gu[:, :tail], gu[:, tail:], pl.ds(full*chunk, tail))
    if with_down:
        o = dot(act_ref[...], wd_ref[...]).astype(BF16)
        h1_ref[...] = h_ref[...] + o

def fwd(layer, h, wg, wu, wd=None, tb=256, chunk=512):
    t, d = h.shape; ff = wg.shape[2]
    once = pl.Buffered(1)
    w_spec = lambda: pl.BlockSpec((None, d, ff), lambda i: (layer, 0, 0), pipeline_mode=once)
    ins = [h, wg, wu]; in_specs = [pl.BlockSpec((tb, d), lambda i: (i, 0)), w_spec(), w_spec()]
    outs = [((d, t), BF16, (d, tb), lambda i: (0, i)), ((t, ff), F32, (tb, ff), lambda i: (i, 0)), ((t, ff), F32, (tb, ff), lambda i: (i, 0)),
            ((ff, t), BF16, (ff, tb), lambda i: (0, i))]
    scratch = [pltpu.VMEM((tb, d), BF16)]
    tail = ff % chunk
    if wd is not None:
        ins.append(wd); in_specs.append(pl.BlockSpec((None, ff, d), lambda i: (layer, 0, 0), pipeline_mode=once))
        outs.append(((t, d), BF16, (tb, d), lambda i: (i, 0)))
        scratch.append(pltpu.VMEM((tb, ff), BF16))
    scratch.append(pltpu.VMEM((d, 2 * tail), BF16))
    n = 3 if wd is not None else 2
    return pl.pallas_call(functools.partial(fwd_kernel, chunk, wd is not None), grid=(t // tb,),
        in_specs=in_specs, out_specs=[pl.BlockSpec(b, m) for _, _, b, m in outs],
        out_shape=[jax.ShapeDtypeStruct(s, dt) for s, dt, _, _ in outs], scratch_shapes=scratch,
        compiler_params=pltpu.CompilerParams(vmem_limit_bytes=61 << 20, dimension_semantics=("arbitrary",)),
        cost_estimate=pl.CostEstimate(flops=2*n*t*d*ff, bytes_accessed=2*n*d*ff+t*ff*10+t*d*6, transcendentals=t*ff), name=f"fwd{layer}")(*ins)

def dwd_kernel(actT_ref, dh_ref, after_ref, o_ref):
    o_ref[...] = dot(actT_ref[...], dh_ref[...]).astype(BF16)

def dwd(actT, dh, after, rb=640, cb=1024):
    ff, t = actT.shape; d = dh.shape[1]
    return pl.pallas_call(dwd_kernel, grid=(d // cb, ff // rb),
        in_specs=[pl.BlockSpec((rb, t), lambda c, r: (r, 0)), pl.BlockSpec((t, cb), lambda c, r: (0, c), pipeline_mode=pl.Buffered(1) if cb == d else None), pl.BlockSpec(memory_space=pl.ANY)],
        out_specs=pl.BlockSpec((rb, cb), lambda c, r: (r, c)), out_shape=jax.ShapeDtypeStruct((ff, d), BF16),
        compiler_params=pltpu.CompilerParams(vmem_limit_bytes=60 << 20, dimension_semantics=("arbitrary","arbitrary")),
        cost_estimate=pl.CostEstimate(flops=2*t*d*ff, bytes_accessed=2*(t*ff+t*d+d*ff), transcendentals=0), name="dwd")(actT, dh, after)

def bwd_kernel(J, nt, ff, sub, keep, gate_ref, up_ref, dh_ref, wd_ref, aT_ref, after_ref, dw_ref, *refs):
    if keep: dgo_ref, duo_ref, dg0, du0, dg1, du1 = refs
    else: dg0, du0, dg1, du1 = refs
    j, t = pl.program_id(0), pl.program_id(1)
    tt = gate_ref.shape[0]
    nfull, tail = ff // J, ff % J
    d = aT_ref.shape[0]; q = d // nt
    rows = pl.ds(pl.multiple_of(t * q, q), q)
    def stage_a(w, put):
        cols = pl.ds(0, w)
        for r in range(tt // sub):
            rs = pl.ds(r * sub, sub)
            dst = pl.ds(pl.multiple_of(t * tt + r * sub, sub), sub)
            dact = dot_nt(dh_ref[rs, :], wd_ref[cols, :]).astype(BF16).astype(F32)
            g = gate_ref[rs, cols]; u = up_ref[rs, cols]
            s = sigmoid(g); silu = g * s
            dup = (dact * silu).astype(BF16)
            dgate = (dact * u * (s + silu * (1.0 - s))).astype(BF16)
            put(dst, dgate, dup)
            if keep: dgo_ref[rs, cols] = dgate; duo_ref[rs, cols] = dup
    def a_full(dg, du):
        def put(dst, a, b): dg[dst, :] = a; du[dst, :] = b
        stage_a(J, put)
    def a_tail(dg):
        def put(dst, a, b): dg[dst, :tail] = a; dg[dst, tail:2*tail] = b
        stage_a(tail, put)
    def b_full(dg, du):
        dw_ref[0] = dot(aT_ref[rows, :], dg[...]).astype(BF16)
        dw_ref[1] = dot(aT_ref[rows, :], du[...]).astype(BF16)
    def b_tail(dg):
        o = dot(aT_ref[rows, :], dg[:, :2*tail]).astype(BF16)
        dw_ref[0, :, :tail] = o[:, :tail]; dw_ref[1, :, :tail] = o[:, tail:]
    odd = lax.rem(j, 2) == 1
    assert nfull % 2 == 0
    @pl.when(j == 0)
    def _(): a_full(dg0, du0)
    @pl.when(odd & (j < nfull))
    def _(): a_full(dg1, du1); b_full(dg0, du0)
    @pl.when(~odd & (j > 0) & (j < nfull))
    def _(): a_full(dg0, du0); b_full(dg1, du1)
    @pl.when(j == nfull)
    def _(): a_tail(dg0); b_full(dg1, du1)
    @pl.when(j == nfull + 1)
    def _(): b_tail(dg0)

def bwd(layer, gate, up, dh, wd, aT, after, J=512, tt=1024, sub=512, keep=True):
    t, ff = gate.shape; d = dh.shape[1]; nt = t // tt; nj = -(-ff // J)
    once = pl.Buffered(1)
    jj = lambda j: jnp.minimum(j, nj - 1)
    ti = lambda j, i: jnp.where(j == nj, nt - 1, i)
    tile = pl.BlockSpec((tt, J), lambda j, i: (ti(j, i), jj(j)))
    in_specs = [tile, tile, pl.BlockSpec((tt, d), lambda j, i: (ti(j, i), 0)), pl.BlockSpec((None, J, d), lambda j, i: (layer, jj(j), 0)),
        pl.BlockSpec((d, t), lambda j, i: (0, 0), pipeline_mode=once), pl.BlockSpec(memory_space=pl.ANY)]
    out_specs = [pl.BlockSpec((2, d // nt, J), lambda j, i: (0, jnp.where(j == 0, 0, i), jnp.maximum(j - 1, 0)))] + [tile] * (2 * keep)
    out_shape = [jax.ShapeDtypeStruct((2, d, ff), BF16)] + [jax.ShapeDtypeStruct((t, ff), BF16)] * (2 * keep)
    return pl.pallas_call(functools.partial(bwd_kernel, J, nt, ff, sub, keep), grid=(nj + 1, nt), in_specs=in_specs,
        out_specs=out_specs, out_shape=out_shape, scratch_shapes=[pltpu.VMEM((t, J), BF16)] * 4,
        compiler_params=pltpu.CompilerParams(vmem_limit_bytes=61 << 20, dimension_semantics=("arbitrary", "arbitrary")),
        cost_estimate=pl.CostEstimate(flops=6*t*d*ff, bytes_accessed=8*t*ff, transcendentals=t*ff), name=f"bwd{layer}")(gate, up, dh, wd, aT, after)

def dx_kernel(n, sub, dg_ref, du_ref, wg_ref, wu_ref, h_ref, dh_ref, o_ref, da_ref):
    i = pl.program_id(0)
    def epi(rs):
        da = da_ref[rs, :].astype(BF16).astype(F32)
        wide = h_ref[rs, :].astype(F32)
        scale = lax.rsqrt(jnp.mean(wide * wide, -1, keepdims=True) + 1e-6)
        mean = jnp.mean(da * wide, -1, keepdims=True)
        dw = da * scale - wide * (scale * scale * scale * mean)
        o_ref[rs, :] = dh_ref[rs, :] + dw.astype(BF16)
    def mm(rs): da_ref[rs, :] = dot_nt(dg_ref[rs, :], wg_ref[...]) + dot_nt(du_ref[rs, :], wu_ref[...])
    blocks = [pl.ds(r * sub, sub) for r in range(dg_ref.shape[0] // sub)]
    @pl.when(i == 0)
    def _():
        for rs in blocks: mm(rs)
    @pl.when((i > 0) & (i < n))
    def _():
        for rs in blocks: epi(rs); mm(rs)
    @pl.when(i == n)
    def _():
        for rs in blocks: epi(rs)

def dx(layer, dg, du, wg, wu, h, dh, tb=512, sub=512):
    t, ff = dg.shape; d = dh.shape[1]; once = pl.Buffered(1); n = t // tb
    cur = lambda i: (jnp.minimum(i, n - 1), 0)
    prv = lambda i: (jnp.maximum(i - 1, 0), 0)
    w_spec = pl.BlockSpec((None, d, ff), lambda i: (layer, 0, 0), pipeline_mode=once)
    return pl.pallas_call(functools.partial(dx_kernel, n, sub), grid=(n + 1,),
        in_specs=[pl.BlockSpec((tb, ff), cur), pl.BlockSpec((tb, ff), cur), w_spec, w_spec, pl.BlockSpec((tb, d), prv), pl.BlockSpec((tb, d), prv)],
        out_specs=pl.BlockSpec((tb, d), prv), out_shape=jax.ShapeDtypeStruct((t, d), BF16), scratch_shapes=[pltpu.VMEM((tb, d), F32)],
        compiler_params=pltpu.CompilerParams(vmem_limit_bytes=60 << 20, dimension_semantics=("arbitrary",)),
        cost_estimate=pl.CostEstimate(flops=4*t*d*ff, bytes_accessed=4*t*ff, transcendentals=0), name=f"dx{layer}")(dg, du, wg, wu, h, dh)

def place_kernel(own_ref, left_ref, right_ref, far0_ref, far1_ref, out_ref, send):
    k = pl.program_id(0)

    @pl.when(k == 0)
    def _():
        out_ref[...] = own_ref[...]

    @pl.when(k == 1)
    def _():
        out_ref[...] = left_ref[...]

    @pl.when(k == 2)
    def _():
        out_ref[...] = right_ref[...]

    @pl.when(k == 3)
    def _():
        out_ref[0] = far0_ref[...]
        out_ref[1] = far1_ref[...]


def place(me, n, own, left, right, far0, far1):
    layers, rows, cols = own.shape
    where = (me + jnp.array([0, n - 1, 1, 2], jnp.int32)) % n

    def body(where_ref, *refs):
        place_kernel(*refs, None)

    def whole(k, where_ref):
        return (0, 0, 0)

    three = pl.BlockSpec((layers, rows, cols), whole)
    two = pl.BlockSpec((rows, cols), lambda k, where_ref: (0, 0))
    return pl.pallas_call(
        body,
        grid_spec=pltpu.PrefetchScalarGridSpec(
            num_scalar_prefetch=1,
            grid=(n,),
            in_specs=[three, three, three, two, two],
            out_specs=pl.BlockSpec((layers, rows, cols), lambda k, where_ref: (0, where_ref[k], 0)),
        ),
        out_shape=jax.ShapeDtypeStruct((layers, n * rows, cols), own.dtype),
        compiler_params=pltpu.CompilerParams(vmem_limit_bytes=40 << 20, dimension_semantics=("arbitrary",)),
        cost_estimate=pl.CostEstimate(flops=0, bytes_accessed=4 * layers * n * rows * cols, transcendentals=0),
        name="place",
    )(where, own, left, right, far0, far1)


def gathered(own, n):
    to_right = [(i, (i + 1) % n) for i in range(n)]
    to_left = [(i, (i - 1) % n) for i in range(n)]
    left = lax.ppermute(own, "dp", to_right)
    right = lax.ppermute(own, "dp", to_left)
    far0 = lax.ppermute(left[0], "dp", to_right)
    far1 = lax.ppermute(right[1], "dp", to_left)
    return place(lax.axis_index("dp"), n, own, left, right, far0, far1)


def adamw(w, m, v, g):
    m = 0.9 * m + 0.1 * g
    v = 0.95 * v + 0.05 * g * g
    step = m * lax.rsqrt(v + 1e-8) + 0.1 * w
    return (w - 0.02 * step).astype(BF16), m, v


def solution(mesh):
    n = mesh.shape["dp"]

    def of_a_device(x, dy, wg, wu, wd, *moments):
        x, dy = x[0], dy[0]
        m, v = moments[:3], moments[3:]
        a0, g0, u0, act0, h1 = fwd(0, x, wg, wu, wd)
        a1, g1, u1, act1 = fwd(1, h1, wg, wu)

        def scattered(t):
            return lax.psum_scatter(t, "dp", scatter_dimension=t.ndim - 2, tiled=True)

        mine = dwd(act1, dy, act1, rb=800)
        dwd1 = scattered(mine)
        dgu1, dg, du = bwd(1, g1, u1, dy, wd, a1, mine, sub=256, keep=True)
        dgu1 = scattered(dgu1)
        dh = dx(1, dg, du, wg, wu, h1, dy)
        mine = dwd(act0, dh, dwd1, rb=800)
        dwd0 = scattered(mine)
        dgu0, = bwd(0, g0, u0, dh, wd, a0, dgu1, sub=256, keep=False)
        dgu0 = scattered(dgu0)
        grads = [jnp.stack(p).astype(F32) for p in ((dgu0[0], dgu1[0]), (dgu0[1], dgu1[1]), (dwd0, dwd1))]
        total = lax.psum(sum(jnp.sum(g * g) for g in grads), "dp")
        count = sum(w.size for w in (wg, wu, wd))
        factor = jnp.minimum(1.0, 0.5 * lax.rsqrt(total / count + 1e-30))
        me = lax.axis_index("dp")
        new = []
        for w, mm, vv, g in zip((wg, wu, wd), m, v, grads):
            rows = g.shape[1]
            own = lax.dynamic_slice_in_dim(w, me * rows, rows, 1)
            new.append(adamw(own.astype(F32), mm, vv, g * factor))
        return tuple(gathered(one[0], n) for one in new) + tuple(one[1] for one in new) + tuple(one[2] for one in new)

    seq = P(("rep", "dp"))
    whole, rows = P(), P(None, "dp")
    return jax.shard_map(
        of_a_device,
        mesh=mesh,
        in_specs=(seq, seq) + (whole,) * 3 + (rows,) * 6,
        out_specs=(P("rep"),) * 3 + (P("rep", "dp"),) * 6,
        check_vma=False,
    )
```

```python
import functools
import jax, jax.numpy as jnp
from jax import lax
from jax.experimental import pallas as pl
from jax.experimental.pallas import tpu as pltpu
from jax.sharding import PartitionSpec as P

F32, BF16 = jnp.float32, jnp.bfloat16
def dot(a, b): return jnp.dot(a, b, preferred_element_type=F32)
def dot_nt(a, b): return lax.dot_general(a, b, (((1,), (1,)), ((), ())), preferred_element_type=F32)
def sigmoid(x): return 0.5 * jnp.tanh(0.5 * x) + 0.5

def fwd_kernel(chunk, with_down, h_ref, wg_ref, wu_ref, *refs):
    if with_down: wd_ref, aT_ref, gate_ref, up_ref, actT_ref, h1_ref, a_ref, act_ref, wt_ref = refs
    else: aT_ref, gate_ref, up_ref, actT_ref, a_ref, wt_ref = refs
    ff = wg_ref.shape[1]; full = ff // chunk; tail = ff - full * chunk
    @pl.when(pl.program_id(0) == 0)
    def _():
        wt_ref[:, :tail] = wg_ref[:, full*chunk:]; wt_ref[:, tail:] = wu_ref[:, full*chunk:]
    wide = h_ref[...].astype(F32)
    scale = lax.rsqrt(jnp.mean(wide * wide, -1, keepdims=True) + 1e-6)
    a = (wide * scale).astype(BF16)
    a_ref[...] = a
    aT_ref[...] = a.T
    def part(g, u, cols):
        gate_ref[:, cols] = g; up_ref[:, cols] = u
        act = (g * sigmoid(g) * u).astype(BF16)
        if with_down: act_ref[:, cols] = act
        actT_ref[cols, :] = act.T
    for c in range(full):
        cols = pl.ds(c * chunk, chunk)
        part(dot(a_ref[...], wg_ref[:, cols]), dot(a_ref[...], wu_ref[:, cols]), cols)
    gu = dot(a_ref[...], wt_ref[...])
    part(gu[:, :tail], gu[:, tail:], pl.ds(full*chunk, tail))
    if with_down:
        o = dot(act_ref[...], wd_ref[...]).astype(BF16)
        h1_ref[...] = h_ref[...] + o

def fwd(layer, h, wg, wu, wd=None, tb=256, chunk=512):
    t, d = h.shape; ff = wg.shape[2]
    once = pl.Buffered(1)
    w_spec = lambda: pl.BlockSpec((None, d, ff), lambda i: (layer, 0, 0), pipeline_mode=once)
    ins = [h, wg, wu]; in_specs = [pl.BlockSpec((tb, d), lambda i: (i, 0)), w_spec(), w_spec()]
    outs = [((d, t), BF16, (d, tb), lambda i: (0, i)), ((t, ff), F32, (tb, ff), lambda i: (i, 0)), ((t, ff), F32, (tb, ff), lambda i: (i, 0)),
            ((ff, t), BF16, (ff, tb), lambda i: (0, i))]
    scratch = [pltpu.VMEM((tb, d), BF16)]
    tail = ff % chunk
    if wd is not None:
        ins.append(wd); in_specs.append(pl.BlockSpec((None, ff, d), lambda i: (layer, 0, 0), pipeline_mode=once))
        outs.append(((t, d), BF16, (tb, d), lambda i: (i, 0)))
        scratch.append(pltpu.VMEM((tb, ff), BF16))
    scratch.append(pltpu.VMEM((d, 2 * tail), BF16))
    n = 3 if wd is not None else 2
    return pl.pallas_call(functools.partial(fwd_kernel, chunk, wd is not None), grid=(t // tb,),
        in_specs=in_specs, out_specs=[pl.BlockSpec(b, m) for _, _, b, m in outs],
        out_shape=[jax.ShapeDtypeStruct(s, dt) for s, dt, _, _ in outs], scratch_shapes=scratch,
        compiler_params=pltpu.CompilerParams(vmem_limit_bytes=61 << 20, dimension_semantics=("arbitrary",)),
        cost_estimate=pl.CostEstimate(flops=2*n*t*d*ff, bytes_accessed=2*n*d*ff+t*ff*10+t*d*6, transcendentals=t*ff), name=f"fwd{layer}")(*ins)

def dwd_kernel(actT_ref, dh_ref, after_ref, o_ref):
    o_ref[...] = dot(actT_ref[...], dh_ref[...]).astype(BF16)

def dwd(actT, dh, after, rb=640, cb=1024):
    ff, t = actT.shape; d = dh.shape[1]
    return pl.pallas_call(dwd_kernel, grid=(d // cb, ff // rb),
        in_specs=[pl.BlockSpec((rb, t), lambda c, r: (r, 0)), pl.BlockSpec((t, cb), lambda c, r: (0, c), pipeline_mode=pl.Buffered(1) if cb == d else None), pl.BlockSpec(memory_space=pl.ANY)],
        out_specs=pl.BlockSpec((rb, cb), lambda c, r: (r, c)), out_shape=jax.ShapeDtypeStruct((ff, d), BF16),
        compiler_params=pltpu.CompilerParams(vmem_limit_bytes=60 << 20, dimension_semantics=("arbitrary","arbitrary")),
        cost_estimate=pl.CostEstimate(flops=2*t*d*ff, bytes_accessed=2*(t*ff+t*d+d*ff), transcendentals=0), name="dwd")(actT, dh, after)


MESH = pl.DeviceIdType.MESH


class Ring:
    def __init__(self, n, jobs, stages, sems, ss_refs):
        self.n, self.jobs, self.stages, self.ss = n, jobs, stages, ss_refs
        self.out_send, self.stage_send, self.arrive, self.load = sems
        self.me = lax.axis_index("dp")

    def enter(self):
        barrier = pltpu.get_barrier_semaphore()
        for k in range(1, self.n):
            pl.semaphore_signal(barrier, inc=1, device_id={"dp": lax.rem(self.me + k, self.n)}, device_id_type=MESH)
        pl.semaphore_wait(barrier, self.n - 1)
        for ss in self.ss:
            ss[...] = jnp.zeros_like(ss)

    def owner(self, h, way):
        return lax.rem(self.me + (2 * self.n - 1 - h if way == 0 else 1 + h), self.n)

    def send(self, k, h, way):
        job = self.jobs[k]
        to = lax.rem(self.me + (1 if way == 0 else self.n - 1), self.n)
        if h == 0:
            src, sem = job["piece"](way, self.owner(0, way)), self.out_send.at[k, way]
        else:
            src, sem = self.staged(k, h, way)[0], self.stage_send.at[job["kind"], k % 2, h - 1, way]
        return pltpu.make_async_remote_copy(
            src_ref=src,
            dst_ref=job["slot"](h, way),
            send_sem=sem,
            recv_sem=self.arrive.at[k, h, way],
            device_id={"dp": to},
            device_id_type=MESH,
        )

    def staged(self, k, h, way):
        kind, wide = self.jobs[k]["kind"], self.jobs[k]["wide"]
        return [stage.at[k % 2, h - 1, way, :, pl.ds(0, wide)] for stage in self.stages[kind]]

    def loads(self, k, h, way):
        job = self.jobs[k]
        came, mine = self.staged(k, h, way)
        sem = self.load.at[job["kind"], k % 2]
        return (
            pltpu.make_async_copy(job["slot"](h - 1, way), came, sem.at[0, h - 1, way]),
            pltpu.make_async_copy(job["piece"](way, self.owner(h, way)), mine, sem.at[1, h - 1, way]),
        )

    def result(self, k, way):
        job = self.jobs[k]
        came, _ = self.staged(k, self.n - 1, way)
        return pltpu.make_async_copy(came, job["out"](way), self.stage_send.at[job["kind"], k % 2, self.n - 2, way])

    def hop_a(self, k, h, before):
        for way in (0, 1):
            if before is not None:
                self.settle(before, h, way)
            self.send(k, h - 1, way).wait_recv()
            for copy in self.loads(k, h, way):
                copy.start()

    def settle(self, k, h, way):
        if h < self.n - 1:
            self.send(k, h, way).wait_send()
        else:
            self.result(k, way).wait()

    def hop_b(self, k, h):
        kind = self.jobs[k]["kind"]
        ss = self.ss[kind]
        for way in (0, 1):
            for copy in self.loads(k, h, way):
                copy.wait()
            came, mine = self.staged(k, h, way)
            wide = self.jobs[k]["wide"]
            rows = 32

            @pl.loop(0, came.shape[0] // rows)
            def _(r):
                at = pl.ds(pl.multiple_of(r * rows, rows), rows)
                total = (came[at, :].astype(F32) + mine[at, :].astype(F32)).astype(BF16)
                came[at, :] = total
                if h == self.n - 1:
                    square = total.astype(F32)
                    square = square * square
                    ss[:, :wide] += sum(square[8 * q : 8 * q + 8] for q in range(rows // 8))

            if h < self.n - 1:
                self.send(k, h, way).start()
            else:
                self.result(k, way).start()

    def plan(self, step_us, slack):
        n, jobs, steps = self.n, self.jobs, len(step_us)
        todo, came, before, gone = [], {}, {}, {}
        link = now = 0.0
        injected, started, left = 0, [], len(jobs) * (n - 1)
        step = 0

        def put(k, h, at):
            nonlocal link
            link = max(link, at) + jobs[k]["us"]
            gone[k, h] = link + 2.0
            if h < n - 1:
                came[k, h + 1] = link + 3.0

        while left:
            inside = step < steps
            if not inside and not started:
                now = max(now, min(came.values(), default=now))
            for k, h in started:
                todo.append((step, "b", k, h, None))
                left -= 1
                if h < n - 1:
                    put(k, h, now + 0.7)
            started = []
            if injected < len(jobs) and (jobs[injected]["ready"] <= step or not inside) and link <= now + 12:
                todo.append((step, "inject", injected, 0, None))
                put(injected, 0, now)
                injected += 1
            due = []
            for (k, h), at in came.items():
                at = max(at, gone.get((before.get((jobs[k]["kind"], k % 2, h)), h), 0.0))
                if at + slack * inside <= now or not inside:
                    due.append((at, (k, h)))
            due.sort()
            for _, (k, h) in due[: 2 if inside else 1]:
                key = jobs[k]["kind"], k % 2, h
                if any((jobs[i]["kind"], i % 2, g) == key for i, g in started):
                    continue
                del came[k, h]
                todo.append((step, "a", k, h, before.get(key)))
                before[key] = k
                started.append((k, h))
            now += step_us[step] if inside else 2.0 if due else 1.0
            step += 1
        self.last = [(k, h) for (_, _, h), k in before.items()]
        return todo

    def do(self, what, k, h, before):
        if what == "inject":
            for way in (0, 1):
                self.send(k, 0, way).start()
        elif what == "a":
            self.hop_a(k, h, before)
        else:
            self.hop_b(k, h)

    def follow(self, plan, step, steps):
        for s in range(steps):
            if any(at == s for at, *_ in plan):

                @pl.when(step == s)
                def _():
                    for at, *what in plan:
                        if at == s:
                            self.do(*what)

    def finish(self, plan, steps):
        for at, *what in plan:
            if at >= steps:
                self.do(*what)

    def leave(self):
        for k, h in self.last:
            for way in (0, 1):
                self.settle(k, h, way)
        for k in range(len(self.jobs)):
            for way in (0, 1):
                self.send(k, 0, way).wait_send()


def ring_sems(n, jobs):
    dma = pltpu.SemaphoreType.DMA
    return [dma((jobs, 2)), dma((2, 2, n - 1, 2)), dma((jobs, n - 1, 2)), dma((2, 2, 2, n - 1, 2))]


LINK = 46.6e3


def down_jobs(n, count, dwd_ref, slots, out_ref):
    rows, cols = dwd_ref.shape[0] // n, dwd_ref.shape[1] // 2
    some = rows // count

    def job(c):
        def at(way):
            return pl.ds(way * cols, cols)

        return dict(
            kind=0,
            ready=0,
            us=2 * some * cols / LINK,
            wide=cols,
            piece=lambda way, owner: dwd_ref.at[pl.ds(pl.multiple_of(owner * rows + c * some, 16), some), at(way)],
            slot=lambda h, way: slots.at[c, h, way],
            out=lambda way: out_ref.at[pl.ds(c * some, some), at(way)],
        )

    return [job(c) for c in range(count)]


def in_jobs(n, spans, dw_ref, slots, out_ref, kind, ready):
    rows = dw_ref.shape[1] // n

    def job(slot, first, wide):
        at = pl.ds(first, wide)
        return dict(
            kind=kind,
            ready=ready(first + wide),
            us=2 * rows * wide / LINK,
            wide=wide,
            piece=lambda way, owner: dw_ref.at[way, pl.ds(pl.multiple_of(owner * rows, 16), rows), at],
            slot=lambda h, way: slots.at[slot, h, way, :, pl.ds(0, wide)],
            out=lambda way: out_ref.at[way, :, at],
        )

    return [job(slot, *span) for slot, span in enumerate(spans)]


def spans_of(cols, wide, first=0, last=None):
    return tuple((c, min(wide, cols - c)) for c in range(0, cols, wide))[first:last]


DOWN_JOBS = 5


def bwd_kernel(cfg, *refs):
    n, J, nt, ff, sub, keep, spans, slack, last = cfg
    gate_ref, up_ref, dh_ref, wd_ref, aT_ref, dwd_ref = refs[:6]
    refs = refs[6:]
    if last:
        other_ref, refs = refs[0], refs[1:]
    dw_ref, slots0, slots1, gd_ref, gg_ref, ss_out = refs[:6]
    refs = refs[6:]
    if keep:
        dgo_ref, duo_ref = refs[:2]
        refs = refs[2:]
    dg0, du0, dg1, du1, piece, piece_sem, came0, mine0, came1, mine1, ss0, ss1 = refs[:12]
    refs = refs[12:]
    sems, refs = refs[:4], refs[4:]
    j, t = pl.program_id(0), pl.program_id(1)
    step = j * nt + t
    tt = gate_ref.shape[0]
    nfull, tail = ff // J, ff % J
    d = aT_ref.shape[0]
    q = d // nt
    rows = pl.ds(pl.multiple_of(t * q, q), q)
    jobs = down_jobs(n, DOWN_JOBS, dwd_ref, slots0, gd_ref) + in_jobs(
        n, spans, dw_ref, slots1, gg_ref, 1, lambda cols: (-(-cols // J) + 1) * nt + 2
    )
    ring = Ring(n, jobs, ((came0, mine0), (came1, mine1)), sems, (ss0, ss1))
    steps = (nfull + 2) * nt
    plan = ring.plan([1.8] * nt + [4.8] * (nt * (nfull - 1)) + [3.4] * nt + [0.9] * nt, slack)
    @pl.when(step == 0)
    def _():
        ring.enter()

    def put_away(parity, way, cols):
        return pltpu.make_async_copy(piece.at[parity, way, :, pl.ds(0, cols.size)], dw_ref.at[way, rows, cols], piece_sem.at[parity, way])

    parity = lax.rem(t, 2)
    ring.follow(plan, step, steps)

    def stage_a(w, put):
        cols = pl.ds(0, w)
        for r in range(tt // sub):
            rs = pl.ds(r * sub, sub)
            dst = pl.ds(pl.multiple_of(t * tt + r * sub, sub), sub)
            dact = dot_nt(dh_ref[rs, :], wd_ref[cols, :]).astype(BF16).astype(F32)
            g = gate_ref[rs, cols]
            u = up_ref[rs, cols]
            s = sigmoid(g)
            silu = g * s
            dup = (dact * silu).astype(BF16)
            dgate = (dact * u * (s + silu * (1.0 - s))).astype(BF16)
            put(dst, dgate, dup)
            if keep:
                dgo_ref[rs, cols] = dgate
                duo_ref[rs, cols] = dup

    def a_full(dg, du):
        def put(dst, a, b):
            dg[dst, :] = a
            du[dst, :] = b

        stage_a(J, put)

    def a_tail(dg):
        def put(dst, a, b):
            dg[dst, :tail] = a
            dg[dst, tail : 2 * tail] = b

        stage_a(tail, put)

    def b_full(dg, du):
        piece[parity, 0] = dot(aT_ref[rows, :], dg[...]).astype(BF16)
        piece[parity, 1] = dot(aT_ref[rows, :], du[...]).astype(BF16)

    def b_tail(dg):
        o = dot(aT_ref[rows, :], dg[:, : 2 * tail]).astype(BF16)
        piece[parity, 0, :, :tail] = o[:, :tail]
        piece[parity, 1, :, :tail] = o[:, tail:]

    full_cols = pl.ds(pl.multiple_of(jnp.maximum(j - 1, 0) * J, J), J)
    tail_cols = pl.ds(nfull * J, tail)

    @pl.when((step >= nt + 2) & (step < (nfull + 1) * nt + 2))
    def _():
        for way in (0, 1):
            put_away(parity, way, pl.ds(0, J)).wait()

    @pl.when(step >= (nfull + 1) * nt + 2)
    def _():
        for way in (0, 1):
            put_away(parity, way, tail_cols).wait()

    odd = lax.rem(j, 2) == 1

    @pl.when(j == 0)
    def _():
        a_full(dg0, du0)

    @pl.when(odd & (j < nfull))
    def _():
        a_full(dg1, du1)
        b_full(dg0, du0)

    @pl.when(~odd & (j > 0) & (j < nfull))
    def _():
        a_full(dg0, du0)
        b_full(dg1, du1)

    @pl.when(j == nfull)
    def _():
        a_tail(dg0)
        b_full(dg1, du1)

    @pl.when(j == nfull + 1)
    def _():
        b_tail(dg0)

    @pl.when((j > 0) & (j <= nfull))
    def _():
        for way in (0, 1):
            put_away(parity, way, full_cols).start()

    @pl.when(j == nfull + 1)
    def _():
        for way in (0, 1):
            put_away(parity, way, tail_cols).start()

    @pl.when(step == steps - 1)
    def _():
        for p in (0, 1):
            for way in (0, 1):
                put_away(p, way, tail_cols).wait()
        ring.finish(plan, steps)
        total = jnp.sum(ss0[...]) + jnp.sum(ss1[...])
        if last:
            all_ss, ss_send, ss_recv = refs
            total = total + other_ref[0, 0]
            all_ss[ring.me] = jnp.full(all_ss.shape[1:], total, F32)
        ring.leave()
        if last:

            def tell(k):
                peer = lax.rem(ring.me + k, n)
                return pltpu.make_async_remote_copy(
                    src_ref=all_ss.at[ring.me],
                    dst_ref=all_ss.at[ring.me],
                    send_sem=ss_send.at[k - 1],
                    recv_sem=ss_recv.at[k - 1],
                    device_id={"dp": peer},
                    device_id_type=MESH,
                )

            for k in range(1, n):
                tell(k).start()
            for k in range(1, n):
                tell(k).wait()
            total = jnp.max(sum(all_ss[k] for k in range(n)))
        ss_out[...] = jnp.full(ss_out.shape, total, F32)


def bwd(layer, n, gate, up, dh, wd, aT, dwd, other=None, J=512, tt=1024, sub=256, spans=(), slack=0.0):
    keep, last = other is None, other is not None
    t, ff = gate.shape
    d = dh.shape[1]
    nt = t // tt
    nj = -(-ff // J)
    once = pl.Buffered(1)

    def jj(j):
        return jnp.minimum(j, nj - 1)

    def ti(j, i):
        return jnp.where(j == nj, nt - 1, i)

    tile = pl.BlockSpec((tt, J), lambda j, i: (ti(j, i), jj(j)))
    anywhere = pl.BlockSpec(memory_space=pl.ANY)
    small = pl.BlockSpec((8, 128), lambda j, i: (0, 0))
    ins = [gate, up, dh, wd, aT, dwd]
    in_specs = [
        tile,
        tile,
        pl.BlockSpec((tt, d), lambda j, i: (ti(j, i), 0)),
        pl.BlockSpec((None, J, d), lambda j, i: (layer, jj(j), 0)),
        pl.BlockSpec((d, t), lambda j, i: (0, 0), pipeline_mode=once),
        anywhere,
    ]
    if last:
        ins.append(other)
        in_specs.append(small)
    wide = max(w for _, w in spans)
    down_rows, down_wide = ff // n // DOWN_JOBS, d // 2
    slots = [(DOWN_JOBS, n - 1, 2, down_rows, down_wide), (len(spans), n - 1, 2, d // n, wide)]
    out_shape = [jax.ShapeDtypeStruct(s, BF16) for s in [(2, d, ff), *slots, (ff // n, d), (2, d // n, ff)]]
    out_shape.append(jax.ShapeDtypeStruct((8, 128), F32))
    out_specs = [anywhere] * 5 + [small]
    if keep:
        out_shape += [jax.ShapeDtypeStruct((t, ff), BF16)] * 2
        out_specs += [tile] * 2
    scratch = [pltpu.VMEM((t, J), BF16)] * 4 + [pltpu.VMEM((2, 2, d // nt, J), BF16), pltpu.SemaphoreType.DMA((2, 2))]
    scratch += [pltpu.VMEM((2, n - 1, 2, down_rows, down_wide), BF16)] * 2 + [pltpu.VMEM((2, n - 1, 2, d // n, wide), BF16)] * 2
    scratch += [pltpu.VMEM((8, down_wide), F32), pltpu.VMEM((8, wide), F32)]
    scratch += ring_sems(n, DOWN_JOBS + len(spans))
    if last:
        scratch += [pltpu.VMEM((n, 8, 128), F32), pltpu.SemaphoreType.DMA((n - 1,)), pltpu.SemaphoreType.DMA((n - 1,))]
    cfg = (n, J, nt, ff, sub, keep, spans, slack, last)
    return pl.pallas_call(
        functools.partial(bwd_kernel, cfg),
        grid=(nj + 1, nt),
        in_specs=in_specs,
        out_specs=out_specs,
        out_shape=out_shape,
        scratch_shapes=scratch,
        compiler_params=pltpu.CompilerParams(
            vmem_limit_bytes=62 << 20, dimension_semantics=("arbitrary", "arbitrary"), collective_id=1 + layer, has_side_effects=True
        ),
        cost_estimate=pl.CostEstimate(flops=6 * t * d * ff, bytes_accessed=8 * t * ff, transcendentals=t * ff),
        name=f"bwd{layer}",
    )(*ins)


def dwd_ring_kernel(n, steps, spans, slack, actT_ref, dh_ref, dw_ref, gg_in, ss_in, o_ref, slots, gg_ref, ss_out, came, mine, ss, *sems):
    i = pl.program_id(0)
    ring = Ring(n, in_jobs(n, spans, dw_ref, slots, gg_ref, 0, lambda cols: 0), ((came, mine),), sems, (ss,))
    plan = ring.plan([3.4] * steps, slack)

    @pl.when(i == 0)
    def _():
        ring.enter()

    ring.follow(plan, i, steps)
    o_ref[...] = dot(actT_ref[...], dh_ref[...]).astype(BF16)

    @pl.when(i == steps - 1)
    def _():
        ring.finish(plan, steps)
        ring.leave()
        ss_out[...] = ss_in[...] + jnp.sum(ss[...])


def dwd_ring(n, actT, dh, dw, gg, ss, spans, rb=320, slack=0.0):
    ff, t = actT.shape
    d = dh.shape[1]
    steps = ff // rb
    wide = max(w for _, w in spans)
    anywhere = pl.BlockSpec(memory_space=pl.ANY)
    small = pl.BlockSpec((8, 128), lambda i: (0, 0))
    return pl.pallas_call(
        functools.partial(dwd_ring_kernel, n, steps, spans, slack),
        grid=(steps,),
        in_specs=[
            pl.BlockSpec((rb, t), lambda i: (i, 0)),
            pl.BlockSpec((t, d), lambda i: (0, 0), pipeline_mode=pl.Buffered(1)),
            anywhere,
            anywhere,
            small,
        ],
        out_specs=[pl.BlockSpec((rb, d), lambda i: (i, 0)), anywhere, anywhere, small],
        out_shape=[
            jax.ShapeDtypeStruct((ff, d), BF16),
            jax.ShapeDtypeStruct((len(spans), n - 1, 2, d // n, wide), BF16),
            jax.ShapeDtypeStruct(gg.shape, BF16),
            jax.ShapeDtypeStruct((8, 128), F32),
        ],
        scratch_shapes=[pltpu.VMEM((2, n - 1, 2, d // n, wide), BF16)] * 2 + [pltpu.VMEM((8, wide), F32)] + ring_sems(n, len(spans)),
        input_output_aliases={3: 2},
        compiler_params=pltpu.CompilerParams(
            vmem_limit_bytes=60 << 20, dimension_semantics=("arbitrary",), collective_id=4, has_side_effects=True
        ),
        cost_estimate=pl.CostEstimate(flops=2 * t * d * ff, bytes_accessed=2 * (t * ff + t * d + d * ff), transcendentals=0),
        name="dwd_ring",
    )(actT, dh, dw, gg, ss)


def dx_kernel(cfg, dg_ref, du_ref, wg_ref, wu_ref, h_ref, dh_ref, dw_ref, gg_in, ss_in, o_ref, slots, gg_ref, ss_out, da_ref, came, mine, ss, *sems):
    n, steps, spans, slack = cfg
    i = pl.program_id(0)
    ring = Ring(n, in_jobs(n, spans, dw_ref, slots, gg_ref, 0, lambda cols: 0), ((came, mine),), sems, (ss,))
    plan = ring.plan([4.2] * steps + [1.0], slack)

    @pl.when(i == 0)
    def _():
        ring.enter()

    ring.follow(plan, i, steps + 1)

    def epi():
        da = da_ref[...].astype(BF16).astype(F32)
        wide = h_ref[...].astype(F32)
        scale = lax.rsqrt(jnp.mean(wide * wide, -1, keepdims=True) + 1e-6)
        mean = jnp.mean(da * wide, -1, keepdims=True)
        dw = da * scale - wide * (scale * scale * scale * mean)
        o_ref[...] = dh_ref[...] + dw.astype(BF16)

    def mm():
        da_ref[...] = dot_nt(dg_ref[...], wg_ref[...]) + dot_nt(du_ref[...], wu_ref[...])

    @pl.when(i == 0)
    def _():
        mm()

    @pl.when((i > 0) & (i < steps))
    def _():
        epi()
        mm()

    @pl.when(i == steps)
    def _():
        epi()
        ring.finish(plan, steps + 1)
        ring.leave()
        ss_out[...] = ss_in[...] + jnp.sum(ss[...])


def dx(layer, n, dg, du, wg, wu, h, dh, dw, gg, ss, tb=256, spans=(), slack=0.0):
    t, ff = dg.shape
    d = dh.shape[1]
    once = pl.Buffered(1)
    steps = t // tb

    def cur(i):
        return (jnp.minimum(i, steps - 1), 0)

    def prv(i):
        return (jnp.maximum(i - 1, 0), 0)

    w_spec = pl.BlockSpec((None, d, ff), lambda i: (layer, 0, 0), pipeline_mode=once)
    anywhere = pl.BlockSpec(memory_space=pl.ANY)
    small = pl.BlockSpec((8, 128), lambda i: (0, 0))
    wide = max(w for _, w in spans)
    cfg = (n, steps, spans, slack)
    return pl.pallas_call(
        functools.partial(dx_kernel, cfg),
        grid=(steps + 1,),
        in_specs=[
            pl.BlockSpec((tb, ff), cur),
            pl.BlockSpec((tb, ff), cur),
            w_spec,
            w_spec,
            pl.BlockSpec((tb, d), prv),
            pl.BlockSpec((tb, d), prv),
            anywhere,
            anywhere,
            small,
        ],
        out_specs=[pl.BlockSpec((tb, d), prv), anywhere, anywhere, small],
        out_shape=[
            jax.ShapeDtypeStruct((t, d), BF16),
            jax.ShapeDtypeStruct((len(spans), n - 1, 2, d // n, wide), BF16),
            jax.ShapeDtypeStruct(gg.shape, BF16),
            jax.ShapeDtypeStruct((8, 128), F32),
        ],
        scratch_shapes=[pltpu.VMEM((tb, d), F32)]
        + [pltpu.VMEM((2, n - 1, 2, d // n, wide), BF16)] * 2
        + [pltpu.VMEM((8, wide), F32)]
        + ring_sems(n, len(spans)),
        input_output_aliases={7: 2},
        compiler_params=pltpu.CompilerParams(
            vmem_limit_bytes=60 << 20, dimension_semantics=("arbitrary",), collective_id=3, has_side_effects=True
        ),
        cost_estimate=pl.CostEstimate(flops=4 * t * d * ff, bytes_accessed=4 * t * ff, transcendentals=0),
        name=f"dx{layer}",
    )(dg, du, wg, wu, h, dh, dw, gg, ss)


def place_kernel(own_ref, left_ref, right_ref, far0_ref, far1_ref, out_ref, send):
    k = pl.program_id(0)

    @pl.when(k == 0)
    def _():
        out_ref[...] = own_ref[...]

    @pl.when(k == 1)
    def _():
        out_ref[...] = left_ref[...]

    @pl.when(k == 2)
    def _():
        out_ref[...] = right_ref[...]

    @pl.when(k == 3)
    def _():
        out_ref[0] = far0_ref[...]
        out_ref[1] = far1_ref[...]


def place(me, n, own, left, right, far0, far1):
    layers, rows, cols = own.shape
    where = (me + jnp.array([0, n - 1, 1, 2], jnp.int32)) % n

    def body(where_ref, *refs):
        place_kernel(*refs, None)

    def whole(k, where_ref):
        return (0, 0, 0)

    three = pl.BlockSpec((layers, rows, cols), whole)
    two = pl.BlockSpec((rows, cols), lambda k, where_ref: (0, 0))
    return pl.pallas_call(
        body,
        grid_spec=pltpu.PrefetchScalarGridSpec(
            num_scalar_prefetch=1,
            grid=(n,),
            in_specs=[three, three, three, two, two],
            out_specs=pl.BlockSpec((layers, rows, cols), lambda k, where_ref: (0, where_ref[k], 0)),
        ),
        out_shape=jax.ShapeDtypeStruct((layers, n * rows, cols), own.dtype),
        compiler_params=pltpu.CompilerParams(vmem_limit_bytes=40 << 20, dimension_semantics=("arbitrary",)),
        cost_estimate=pl.CostEstimate(flops=0, bytes_accessed=4 * layers * n * rows * cols, transcendentals=0),
        name="place",
    )(where, own, left, right, far0, far1)


def gathered(own, n):
    to_right = [(i, (i + 1) % n) for i in range(n)]
    to_left = [(i, (i - 1) % n) for i in range(n)]
    left = lax.ppermute(own, "dp", to_right)
    right = lax.ppermute(own, "dp", to_left)
    far0 = lax.ppermute(left[0], "dp", to_right)
    far1 = lax.ppermute(right[1], "dp", to_left)
    return place(lax.axis_index("dp"), n, own, left, right, far0, far1)


def adamw(w, m, v, g):
    m = 0.9 * m + 0.1 * g
    v = 0.95 * v + 0.05 * g * g
    step = m * lax.rsqrt(v + 1e-8) + 0.1 * w
    return (w - 0.02 * step).astype(BF16), m, v


def solution(mesh):
    n = mesh.shape["dp"]

    def of_a_device(x, dy, wg, wu, wd, *moments):
        x, dy = x[0], dy[0]
        m, v = moments[:3], moments[3:]
        a0, g0, u0, act0, h1 = fwd(0, x, wg, wu, wd)
        a1, g1, u1, act1 = fwd(1, h1, wg, wu)

        ff = wg.shape[2]
        mine = dwd(act1, dy, act1, rb=800)
        dw1, _, _, gd1, gg1, ss, dg, du = bwd(1, n, g1, u1, dy, wd, a1, mine, spans=spans_of(ff, 512, 0, 2), slack=2.0)
        dh, _, gg1, ss = dx(1, n, dg, du, wg, wu, h1, dy, dw1, gg1, ss, spans=spans_of(ff, 512, 2, 5), slack=1.0)
        mine, _, gg1, ss = dwd_ring(n, act0, dh, dw1, gg1, ss, spans_of(ff, 512, 5))
        _, _, _, gd0, gg0, ss = bwd(0, n, g0, u0, dh, wd, a0, mine, ss, spans=spans_of(ff, 256))
        grads = [jnp.stack(p).astype(F32) for p in ((gg0[0], gg1[0]), (gg0[1], gg1[1]), (gd0, gd1))]
        count = sum(w.size for w in (wg, wu, wd))
        factor = jnp.minimum(1.0, 0.5 * lax.rsqrt(ss[0, 0] / count + 1e-30))
        me = lax.axis_index("dp")
        new = []
        for w, mm, vv, g in zip((wg, wu, wd), m, v, grads):
            rows = g.shape[1]
            own = lax.dynamic_slice_in_dim(w, me * rows, rows, 1)
            new.append(adamw(own.astype(F32), mm, vv, g * factor))
        return tuple(gathered(one[0], n) for one in new) + tuple(one[1] for one in new) + tuple(one[2] for one in new)

    seq = P(("rep", "dp"))
    whole, rows = P(), P(None, "dp")
    return jax.shard_map(
        of_a_device,
        mesh=mesh,
        in_specs=(seq, seq) + (whole,) * 3 + (rows,) * 6,
        out_specs=(P("rep"),) * 3 + (P("rep", "dp"),) * 6,
        check_vma=False,
    )
```

```python
import functools
import jax, jax.numpy as jnp
from jax import lax
from jax.experimental import pallas as pl
from jax.experimental.pallas import tpu as pltpu
from jax.sharding import PartitionSpec as P

N0, N1, N2 = range(3)
F32, BF16 = jnp.float32, jnp.bfloat16
def dot(a, b): return jnp.dot(a, b, preferred_element_type=F32)
def dot_nt(a, b): return lax.dot_general(a, b, (((N1,), (N1,)), ((), ())), preferred_element_type=F32)
def sigmoid(x): return 0.5 * jnp.tanh(0.5 * x) + 0.5

MESH = pl.DeviceIdType.MESH
EARLY_ROWS, ROWS = 480, 160


def meet(n):
    me = lax.axis_index("dp")
    barrier = pltpu.get_barrier_semaphore()
    for k in range(N1, n):
        pl.semaphore_signal(barrier, inc=N1, device_id={"dp": lax.rem(me + k, n)}, device_id_type=MESH)
    pl.semaphore_wait(barrier, n - N1)


def to_neighbours(n, moves, send, recv):
    me = lax.axis_index("dp")
    return [
        pltpu.make_async_remote_copy(
            src_ref=src,
            dst_ref=dst,
            send_sem=send.at[i],
            recv_sem=recv.at[i],
            device_id={"dp": lax.rem(me + (N1 if way == N0 else n - N1), n)},
            device_id_type=MESH,
        )
        for i, (src, dst, way) in enumerate(moves)
    ]


def fwd_kernel(chunk, with_down, n, steps, h_ref, wg_ref, wu_ref, *refs):
    if with_down:
        wd_ref, m_ref, v_ref, aT_ref, gate_ref, up_ref, actT_ref, h1_ref, moved_ref, a_ref, act_ref, wt_ref, send, recv = refs
        layer, here = m_ref.shape[N0] - N1, pl.ds(N0, EARLY_ROWS)
        moves = [(t.at[layer, here], moved_ref.at[way, kind], way) for kind, t in enumerate((m_ref, v_ref)) for way in (N0, N1)]
    else:
        near_ref, aT_ref, gate_ref, up_ref, actT_ref, moved_ref, a_ref, wt_ref, send, recv = refs
        moves = [(near_ref.at[way, way], moved_ref.at[way], way) for way in (N0, N1)]
    copies = to_neighbours(n, moves, send, recv)

    @pl.when(pl.program_id(N0) == N0)
    def _():
        meet(n)
        for copy in copies:
            copy.start()

    @pl.when(pl.program_id(N0) == steps - N1)
    def _():
        for copy in copies:
            copy.wait()

    ff = wg_ref.shape[N1]; full = ff // chunk; tail = ff - full * chunk
    @pl.when(pl.program_id(N0) == N0)
    def _():
        wt_ref[:, :tail] = wg_ref[:, full*chunk:]; wt_ref[:, tail:] = wu_ref[:, full*chunk:]
    wide = h_ref[...].astype(F32)
    scale = lax.rsqrt(jnp.mean(wide * wide, -N1, keepdims=True) + 1e-6)
    a = (wide * scale).astype(BF16)
    a_ref[...] = a
    aT_ref[...] = a.T
    def part(g, u, cols):
        gate_ref[:, cols] = g; up_ref[:, cols] = u
        act = (g * sigmoid(g) * u).astype(BF16)
        if with_down: act_ref[:, cols] = act
        actT_ref[cols, :] = act.T
    for c in range(full):
        cols = pl.ds(c * chunk, chunk)
        part(dot(a_ref[...], wg_ref[:, cols]), dot(a_ref[...], wu_ref[:, cols]), cols)
    gu = dot(a_ref[...], wt_ref[...])
    part(gu[:, :tail], gu[:, tail:], pl.ds(full*chunk, tail))
    if with_down:
        o = dot(act_ref[...], wd_ref[...]).astype(BF16)
        h1_ref[...] = h_ref[...] + o

def fwd(layer, n_dp, h, wg, wu, wd=None, moving=(), tb=256, chunk=512):
    t, d = h.shape; ff = wg.shape[N2]
    once = pl.Buffered(N1)
    w_spec = lambda: pl.BlockSpec((None, d, ff), lambda i: (layer, N0, N0), pipeline_mode=once)
    ins = [h, wg, wu]; in_specs = [pl.BlockSpec((tb, d), lambda i: (i, N0)), w_spec(), w_spec()]
    outs = [((d, t), BF16, (d, tb), lambda i: (N0, i)), ((t, ff), F32, (tb, ff), lambda i: (i, N0)), ((t, ff), F32, (tb, ff), lambda i: (i, N0)),
            ((ff, t), BF16, (ff, tb), lambda i: (N0, i))]
    scratch = [pltpu.VMEM((tb, d), BF16)]
    tail = ff % chunk
    if wd is not None:
        ins.append(wd); in_specs.append(pl.BlockSpec((None, ff, d), lambda i: (layer, N0, N0), pipeline_mode=once))
        outs.append(((t, d), BF16, (tb, d), lambda i: (i, N0)))
        scratch.append(pltpu.VMEM((tb, ff), BF16))
    scratch.append(pltpu.VMEM((d, N2 * tail), BF16))
    ins += moving
    anywhere = pl.BlockSpec(memory_space=pl.ANY)
    in_specs += [anywhere] * len(moving)
    moved = ((N2, N2, EARLY_ROWS, d) if wd is not None else (N2, EARLY_ROWS, d), F32, None, None)
    outs.append(moved)
    scratch += [pltpu.SemaphoreType.DMA((4,))] * N2
    n = 3 if wd is not None else N2
    return pl.pallas_call(functools.partial(fwd_kernel, chunk, wd is not None, n_dp, t // tb), grid=(t // tb,),
        in_specs=in_specs, out_specs=[anywhere if b is None else pl.BlockSpec(b, m) for _, _, b, m in outs],
        out_shape=[jax.ShapeDtypeStruct(s, dt) for s, dt, _, _ in outs], scratch_shapes=scratch,
        compiler_params=pltpu.CompilerParams(vmem_limit_bytes=61 << 20, dimension_semantics=("arbitrary",), collective_id=5 + layer, has_side_effects=True),
        cost_estimate=pl.CostEstimate(flops=N2*n*t*d*ff, bytes_accessed=N2*n*d*ff+t*ff*10+t*d*6, transcendentals=t*ff), name=f"fwd{layer}")(*ins)

def dwd_kernel(actT_ref, dh_ref, *refs):
    o_ref = refs[-N1]
    half = o_ref.shape[N1] // N2

    @pl.loop(N0, N2)
    def _(part):
        cols = pl.ds(pl.multiple_of(part * half, 128), half)
        o_ref[:, cols] = dot(actT_ref[...], dh_ref[:, cols]).astype(BF16)

def dwd(actT, dh, after, rb=640, cb=1024):
    ff, t = actT.shape; d = dh.shape[N1]
    return pl.pallas_call(dwd_kernel, grid=(d // cb, ff // rb),
        in_specs=[pl.BlockSpec((rb, t), lambda c, r: (r, N0)), pl.BlockSpec((t, cb), lambda c, r: (N0, c), pipeline_mode=pl.Buffered(N1) if cb == d else None), *[pl.BlockSpec(memory_space=pl.ANY)] * len(after)],
        out_specs=pl.BlockSpec((rb, cb), lambda c, r: (r, c)), out_shape=jax.ShapeDtypeStruct((ff, d), BF16),
        compiler_params=pltpu.CompilerParams(vmem_limit_bytes=60 << 20, dimension_semantics=("arbitrary","arbitrary")),
        cost_estimate=pl.CostEstimate(flops=N2*t*d*ff, bytes_accessed=N2*(t*ff+t*d+d*ff), transcendentals=N0), name="dwd")(actT, dh, *after)


class Ring:
    def __init__(self, n, jobs, stages, sems, ss_refs):
        self.n, self.jobs, self.stages, self.ss = n, jobs, stages, ss_refs
        self.out_send, self.stage_send, self.arrive, self.load = sems
        self.me = lax.axis_index("dp")

    def enter(self):
        meet(self.n)
        for ss in self.ss:
            ss[...] = jnp.zeros_like(ss)

    def owner(self, h, way):
        return lax.rem(self.me + jnp.where(way == N0, N2 * self.n - N1 - h, N1 + h), self.n)

    def send(self, k, h, way):
        job = self.jobs[k]
        to = lax.rem(self.me + jnp.where(way == N0, N1, self.n - N1), self.n)
        if h == N0:
            src, sem = job["piece"](way, self.owner(N0, way)), self.out_send.at[k, way]
        else:
            src, sem = self.staged(k, h, way)[N0], self.stage_send.at[job["kind"], k % N2, h - N1, way]
        return pltpu.make_async_remote_copy(
            src_ref=src,
            dst_ref=job["slot"](h, way),
            send_sem=sem,
            recv_sem=self.arrive.at[k, h, way],
            device_id={"dp": to},
            device_id_type=MESH,
        )

    def staged(self, k, h, way):
        kind, wide = self.jobs[k]["kind"], self.jobs[k]["wide"]
        return [stage.at[k % N2, h - N1, way, :, pl.ds(N0, wide)] for stage in self.stages[kind]]

    def loads(self, k, h, way):
        job = self.jobs[k]
        came, mine = self.staged(k, h, way)
        sem = self.load.at[job["kind"], k % N2]
        return (
            pltpu.make_async_copy(job["slot"](h - N1, way), came, sem.at[N0, h - N1, way]),
            pltpu.make_async_copy(job["piece"](way, self.owner(h, way)), mine, sem.at[N1, h - N1, way]),
        )

    def result(self, k, way):
        job = self.jobs[k]
        came, _ = self.staged(k, self.n - N1, way)
        return pltpu.make_async_copy(came, job["out"](way), self.stage_send.at[job["kind"], k % N2, self.n - N2, way])

    def hop_a(self, k, h, before):
        @pl.loop(N0, N2)
        def _(way):
            if before is not None:
                self.settle(before, h, way)
            self.send(k, h - N1, way).wait_recv()
            for copy in self.loads(k, h, way):
                copy.start()

    def settle(self, k, h, way):
        if h < self.n - N1:
            self.send(k, h, way).wait_send()
        else:
            self.result(k, way).wait()

    def hop_b(self, k, h):
        kind = self.jobs[k]["kind"]
        ss = self.ss[kind]
        wide = self.jobs[k]["wide"]
        rows = 32

        @pl.loop(N0, N2)
        def _(way):
            for copy in self.loads(k, h, way):
                copy.wait()
            came, mine = self.staged(k, h, way)

            @pl.loop(N0, came.shape[N0] // rows)
            def _(r):
                at = pl.ds(pl.multiple_of(r * rows, rows), rows)
                total = (came[at, :].astype(F32) + mine[at, :].astype(F32)).astype(BF16)
                came[at, :] = total
                if h == self.n - N1:
                    square = total.astype(F32)
                    square = square * square
                    ss[:, :wide] += sum(square[8 * q : 8 * q + 8] for q in range(rows // 8))

            if h < self.n - N1:
                self.send(k, h, way).start()
            else:
                self.result(k, way).start()

    def plan(self, step_us, slack, busy=0.0):
        n, jobs, steps = self.n, self.jobs, len(step_us)
        todo, came, before, gone = [], {}, {}, {}
        link, now = busy, 0.0
        injected, started, left = N0, [], len(jobs) * (n - N1)
        step = N0

        def put(k, h, at):
            nonlocal link
            link = max(link, at) + jobs[k]["us"]
            gone[k, h] = link + 2.0
            if h < n - N1:
                came[k, h + N1] = link + 3.0

        while left:
            inside = step < steps
            if not inside and not started:
                now = max(now, min(came.values(), default=now))
            for k, h in started:
                todo.append((step, "b", k, h, None))
                left -= N1
                if h < n - N1:
                    put(k, h, now + 0.7)
            started = []
            if injected < len(jobs) and (jobs[injected]["ready"] <= step or not inside) and link <= now + 12 + busy:
                todo.append((step, "inject", injected, N0, None))
                put(injected, N0, now)
                injected += N1
            due = []
            for (k, h), at in came.items():
                at = max(at, gone.get((before.get((jobs[k]["kind"], k % N2, h)), h), 0.0))
                if at + slack * inside <= now or not inside:
                    due.append((at, (k, h)))
            due.sort()
            for _, (k, h) in due[: N2 if inside else N1]:
                key = jobs[k]["kind"], k % N2, h
                if any((jobs[i]["kind"], i % N2, g) == key for i, g in started):
                    continue
                del came[k, h]
                todo.append((step, "a", k, h, before.get(key)))
                before[key] = k
                started.append((k, h))
            now += step_us[step] if inside else 2.0 if due else 1.0
            step += N1
        self.last = [(k, h) for (_, _, h), k in before.items()]
        return todo

    def do(self, what, k, h, before):
        if what == "inject":

            @pl.loop(N0, N2)
            def _(way):
                self.send(k, N0, way).start()

        elif what == "a":
            self.hop_a(k, h, before)
        else:
            self.hop_b(k, h)

    def follow(self, plan, step, steps):
        for s in range(steps):
            if any(at == s for at, *_ in plan):

                @pl.when(step == s)
                def _():
                    for at, *what in plan:
                        if at == s:
                            self.do(*what)

    def finish(self, plan, steps):
        for at, *what in plan:
            if at >= steps:
                self.do(*what)

    def leave(self):
        @pl.loop(N0, N2)
        def _(way):
            for k, h in self.last:
                self.settle(k, h, way)
            for k in range(len(self.jobs)):
                self.send(k, N0, way).wait_send()


def ring_sems(n, jobs):
    dma = pltpu.SemaphoreType.DMA
    return [dma((jobs, N2)), dma((N2, N2, n - N1, N2)), dma((jobs, n - N1, N2)), dma((N2, N2, N2, n - N1, N2))]


LINK = 46.6e3


def down_jobs(n, count, dwd_ref, slots, out_ref):
    rows, cols = dwd_ref.shape[N0] // n, dwd_ref.shape[N1] // N2
    some = rows // count

    def job(c):
        def at(way):
            return pl.ds(pl.multiple_of(way * cols, 128), cols)

        return dict(
            kind=N0,
            ready=N0,
            us=N2 * some * cols / LINK,
            wide=cols,
            piece=lambda way, owner: dwd_ref.at[pl.ds(pl.multiple_of(owner * rows + c * some, 16), some), at(way)],
            slot=lambda h, way: slots.at[c, h, way],
            out=lambda way: out_ref.at[pl.ds(c * some, some), at(way)],
        )

    return [job(c) for c in range(count)]


def in_jobs(n, spans, dw_ref, slots, out_ref, kind, ready):
    rows = dw_ref.shape[N1] // n

    def job(slot, first, wide):
        at = pl.ds(first, wide)
        return dict(
            kind=kind,
            ready=ready(first + wide),
            us=N2 * rows * wide / LINK,
            wide=wide,
            piece=lambda way, owner: dw_ref.at[way, pl.ds(pl.multiple_of(owner * rows, 16), rows), at],
            slot=lambda h, way: slots.at[slot, h, way, :, pl.ds(N0, wide)],
            out=lambda way: out_ref.at[way, :, at],
        )

    return [job(slot, *span) for slot, span in enumerate(spans)]


def spans_of(cols, wide, first=N0, last=None):
    return tuple((c, min(wide, cols - c)) for c in range(N0, cols, wide))[first:last]


DOWN_JOBS = 5


def bwd_kernel(cfg, *refs):
    n, J, nt, ff, sub, keep, spans, slack, last, n_after = cfg
    gate_ref, up_ref, dh_ref, wd_ref, aT_ref, dwd_ref = refs[:6]
    refs = refs[6:]
    if last:
        other_ref, refs = refs[N0], refs[N1:]
    refs = refs[n_after:]
    dw_ref, slots0, slots1, gd_ref, gg_ref, ss_out = refs[:6]
    refs = refs[6:]
    if keep:
        dgo_ref, duo_ref = refs[:N2]
        refs = refs[N2:]
    dgu, piece, piece_sem, came0, mine0, came1, mine1, ss0, ss1 = refs[:9]
    refs = refs[9:]
    sems, refs = refs[:4], refs[4:]
    j, t = pl.program_id(N0), pl.program_id(N1)
    step = j * nt + t
    tt = gate_ref.shape[N0]
    nfull, tail = ff // J, ff % J
    d = aT_ref.shape[N0]
    q = d // nt
    rows = pl.ds(pl.multiple_of(t * q, q), q)
    jobs = down_jobs(n, DOWN_JOBS, dwd_ref, slots0, gd_ref) + in_jobs(
        n, spans, dw_ref, slots1, gg_ref, N1, lambda cols: (-(-cols // J) + N1) * nt + N2
    )
    ring = Ring(n, jobs, ((came0, mine0), (came1, mine1)), sems, (ss0, ss1))
    steps = (nfull + N2) * nt
    plan = ring.plan([1.8] * nt + [4.8] * (nt * (nfull - N1)) + [3.4] * nt + [0.9] * nt, slack)
    @pl.when(step == N0)
    def _():
        ring.enter()

    def put_away(parity, way, cols):
        return pltpu.make_async_copy(piece.at[parity, way, :, pl.ds(N0, cols.size)], dw_ref.at[way, rows, cols], piece_sem.at[parity, way])

    parity = lax.rem(t, N2)
    ring.follow(plan, step, steps)

    slot = lax.rem(j, N2)
    other = N1 - slot

    def stage_a(part, w, put):
        cols = pl.ds(N0, w)
        for r in range(tt // sub // N2):
            first = pl.multiple_of(part * (tt // N2) + r * sub, sub)
            rs = pl.ds(first, sub)
            dst = pl.ds(pl.multiple_of(t * tt + first, sub), sub)
            dact = dot_nt(dh_ref[rs, :], wd_ref[cols, :]).astype(BF16).astype(F32)
            g = gate_ref[rs, cols]
            u = up_ref[rs, cols]
            s = sigmoid(g)
            silu = g * s
            dup = (dact * silu).astype(BF16)
            dgate = (dact * u * (s + silu * (1.0 - s))).astype(BF16)
            put(dst, dgate, dup)
            if keep:
                dgo_ref[rs, cols] = dgate
                duo_ref[rs, cols] = dup

    def a_full(part):
        def put(dst, a, b):
            dgu[slot, N0, dst, :] = a
            dgu[slot, N1, dst, :] = b

        stage_a(part, J, put)

    def a_tail(part):
        def put(dst, a, b):
            dgu[slot, N0, dst, :tail] = a
            dgu[slot, N0, dst, tail : N2 * tail] = b

        stage_a(part, tail, put)

    def b_full(part):
        piece[parity, part] = dot(aT_ref[rows, :], dgu[other, part]).astype(BF16)

    def b_tail():
        o = dot(aT_ref[rows, :], dgu[other, N0, :, : N2 * tail]).astype(BF16)
        piece[parity, N0, :, :tail] = o[:, :tail]
        piece[parity, N1, :, :tail] = o[:, tail:]

    full_cols = pl.ds(pl.multiple_of(jnp.maximum(j - N1, N0) * J, J), J)
    tail_cols = pl.ds(nfull * J, tail)

    @pl.when((step >= nt + N2) & (step < (nfull + N1) * nt + N2))
    def _():
        for way in (N0, N1):
            put_away(parity, way, pl.ds(N0, J)).wait()

    @pl.when(step >= (nfull + N1) * nt + N2)
    def _():
        for way in (N0, N1):
            put_away(parity, way, tail_cols).wait()

    @pl.when(j == N0)
    def _():
        pl.loop(N0, N2)(a_full)

    @pl.when((j > N0) & (j < nfull))
    def _():
        @pl.loop(N0, N2)
        def _(part):
            b_full(part)
            a_full(part)

    @pl.when(j == nfull)
    def _():
        @pl.loop(N0, N2)
        def _(part):
            b_full(part)
            a_tail(part)

    @pl.when(j == nfull + N1)
    def _():
        b_tail()

    @pl.when((j > N0) & (j <= nfull))
    def _():
        for way in (N0, N1):
            put_away(parity, way, full_cols).start()

    @pl.when(j == nfull + N1)
    def _():
        for way in (N0, N1):
            put_away(parity, way, tail_cols).start()

    @pl.when(step == steps - N1)
    def _():
        for p in (N0, N1):
            for way in (N0, N1):
                put_away(p, way, tail_cols).wait()
        ring.finish(plan, steps)
        total = jnp.sum(ss0[...]) + jnp.sum(ss1[...])
        if last:
            all_ss, ss_send, ss_recv = refs
            total = total + other_ref[N0, N0]
            all_ss[ring.me] = jnp.full(all_ss.shape[N1:], total, F32)
        ring.leave()
        if last:

            def tell(k):
                peer = lax.rem(ring.me + k, n)
                return pltpu.make_async_remote_copy(
                    src_ref=all_ss.at[ring.me],
                    dst_ref=all_ss.at[ring.me],
                    send_sem=ss_send.at[k - N1],
                    recv_sem=ss_recv.at[k - N1],
                    device_id={"dp": peer},
                    device_id_type=MESH,
                )

            for k in range(N1, n):
                tell(k).start()
            for k in range(N1, n):
                tell(k).wait()
            total = jnp.max(sum(all_ss[k] for k in range(n)))
        ss_out[...] = jnp.full(ss_out.shape, total, F32)


def bwd(layer, n, gate, up, dh, wd, aT, dwd, other=None, after=(), J=512, tt=1024, sub=256, spans=(), slack=0.0):
    keep, last = other is None, other is not None
    t, ff = gate.shape
    d = dh.shape[N1]
    nt = t // tt
    nj = -(-ff // J)
    once = pl.Buffered(N1)

    def jj(j):
        return jnp.minimum(j, nj - N1)

    def ti(j, i):
        return jnp.where(j == nj, nt - N1, i)

    tile = pl.BlockSpec((tt, J), lambda j, i: (ti(j, i), jj(j)))
    anywhere = pl.BlockSpec(memory_space=pl.ANY)
    small = pl.BlockSpec((8, 128), lambda j, i: (N0, N0))
    ins = [gate, up, dh, wd, aT, dwd]
    in_specs = [
        tile,
        tile,
        pl.BlockSpec((tt, d), lambda j, i: (ti(j, i), N0)),
        pl.BlockSpec((None, J, d), lambda j, i: (layer, jj(j), N0)),
        pl.BlockSpec((d, t), lambda j, i: (N0, N0), pipeline_mode=once),
        anywhere,
    ]
    if last:
        ins.append(other)
        in_specs.append(small)
    ins += after
    in_specs += [anywhere] * len(after)
    wide = max(w for _, w in spans)
    down_rows, down_wide = ff // n // DOWN_JOBS, d // N2
    slots = [(DOWN_JOBS, n - N1, N2, down_rows, down_wide), (len(spans), n - N1, N2, d // n, wide)]
    out_shape = [jax.ShapeDtypeStruct(s, BF16) for s in [(N2, d, ff), *slots, (ff // n, d), (N2, d // n, ff)]]
    out_shape.append(jax.ShapeDtypeStruct((8, 128), F32))
    out_specs = [anywhere] * 5 + [small]
    if keep:
        out_shape += [jax.ShapeDtypeStruct((t, ff), BF16)] * N2
        out_specs += [tile] * N2
    scratch = [pltpu.VMEM((N2, N2, t, J), BF16)] + [pltpu.VMEM((N2, N2, d // nt, J), BF16), pltpu.SemaphoreType.DMA((N2, N2))]
    scratch += [pltpu.VMEM((N2, n - N1, N2, down_rows, down_wide), BF16)] * N2 + [pltpu.VMEM((N2, n - N1, N2, d // n, wide), BF16)] * N2
    scratch += [pltpu.VMEM((8, down_wide), F32), pltpu.VMEM((8, wide), F32)]
    scratch += ring_sems(n, DOWN_JOBS + len(spans))
    if last:
        scratch += [pltpu.VMEM((n, 8, 128), F32), pltpu.SemaphoreType.DMA((n - N1,)), pltpu.SemaphoreType.DMA((n - N1,))]
    cfg = (n, J, nt, ff, sub, keep, spans, slack, last, len(after))
    return pl.pallas_call(
        functools.partial(bwd_kernel, cfg),
        grid=(nj + N1, nt),
        in_specs=in_specs,
        out_specs=out_specs,
        out_shape=out_shape,
        scratch_shapes=scratch,
        compiler_params=pltpu.CompilerParams(
            vmem_limit_bytes=62 << 20, dimension_semantics=("arbitrary", "arbitrary"), collective_id=N1 + layer, has_side_effects=True
        ),
        cost_estimate=pl.CostEstimate(flops=6 * t * d * ff, bytes_accessed=8 * t * ff, transcendentals=t * ff),
        name=f"bwd{layer}",
    )(*ins)


def dwd_ring_kernel(n, steps, spans, slack, actT_ref, dh_ref, dw_ref, gg_in, ss_in, near_ref, *refs):
    o_ref, slots, gg_ref, ss_out, far_ref, came, mine, ss, *sems, send, recv = refs
    half = EARLY_ROWS // N2
    parts = [pl.ds(way * half, half) for way in (N0, N1)]
    copies = to_neighbours(n, [(near_ref.at[way, parts[way]], far_ref.at[parts[way]], way) for way in (N0, N1)], send, recv)
    i = pl.program_id(N0)
    ring = Ring(n, in_jobs(n, spans, dw_ref, slots, gg_ref, N0, lambda cols: N0), ((came, mine),), sems, (ss,))
    plan = ring.plan([3.4] * steps, slack)

    @pl.when(i == N0)
    def _():
        ring.enter()

    @pl.when(i == steps // N2)
    def _():
        for copy in copies:
            copy.start()

    ring.follow(plan, i, steps)
    o_ref[...] = dot(actT_ref[...], dh_ref[...]).astype(BF16)

    @pl.when(i == steps - N1)
    def _():
        ring.finish(plan, steps)
        ring.leave()
        for copy in copies:
            copy.wait()
        ss_out[...] = ss_in[...] + jnp.sum(ss[...])


def dwd_ring(n, actT, dh, dw, gg, ss, near, spans, rb=320, slack=0.0):
    ff, t = actT.shape
    d = dh.shape[N1]
    steps = ff // rb
    wide = max(w for _, w in spans)
    anywhere = pl.BlockSpec(memory_space=pl.ANY)
    small = pl.BlockSpec((8, 128), lambda i: (N0, N0))
    return pl.pallas_call(
        functools.partial(dwd_ring_kernel, n, steps, spans, slack),
        grid=(steps,),
        in_specs=[
            pl.BlockSpec((rb, t), lambda i: (i, N0)),
            pl.BlockSpec((t, d), lambda i: (N0, N0), pipeline_mode=pl.Buffered(N1)),
            anywhere,
            anywhere,
            small,
            anywhere,
        ],
        out_specs=[pl.BlockSpec((rb, d), lambda i: (i, N0)), anywhere, anywhere, small, anywhere],
        out_shape=[
            jax.ShapeDtypeStruct((ff, d), BF16),
            jax.ShapeDtypeStruct((len(spans), n - N1, N2, d // n, wide), BF16),
            jax.ShapeDtypeStruct(gg.shape, BF16),
            jax.ShapeDtypeStruct((8, 128), F32),
            jax.ShapeDtypeStruct((EARLY_ROWS, d), BF16),
        ],
        scratch_shapes=[pltpu.VMEM((N2, n - N1, N2, d // n, wide), BF16)] * N2 + [pltpu.VMEM((8, wide), F32)] + ring_sems(n, len(spans)) + [pltpu.SemaphoreType.DMA((N2,))] * N2,
        input_output_aliases={3: N2},
        compiler_params=pltpu.CompilerParams(
            vmem_limit_bytes=60 << 20, dimension_semantics=("arbitrary",), collective_id=4, has_side_effects=True
        ),
        cost_estimate=pl.CostEstimate(flops=N2 * t * d * ff, bytes_accessed=N2 * (t * ff + t * d + d * ff), transcendentals=N0),
        name="dwd_ring",
    )(actT, dh, dw, gg, ss, near)


def dx_kernel(cfg, dg_ref, du_ref, wg_ref, wu_ref, h_ref, dh_ref, dw_ref, gg_in, ss_in, gd_ref, *refs):
    n, steps, spans, slack = cfg
    o_ref, slots, gg_ref, ss_out, near_ref, da_ref, came, mine, ss, *sems, send, recv = refs
    copies = to_neighbours(n, [(gd_ref.at[pl.ds(N0, EARLY_ROWS)], near_ref.at[way], way) for way in (N0, N1)], send, recv)
    i = pl.program_id(N0)
    ring = Ring(n, in_jobs(n, spans, dw_ref, slots, gg_ref, N0, lambda cols: N0), ((came, mine),), sems, (ss,))
    plan = ring.plan([4.2] * steps + [1.0], slack, N2 * EARLY_ROWS * gd_ref.shape[N1] / LINK)

    @pl.when(i == N0)
    def _():
        ring.enter()
        for copy in copies:
            copy.start()

    ring.follow(plan, i, steps + N1)

    def epi():
        da = da_ref[...].astype(BF16).astype(F32)
        wide = h_ref[...].astype(F32)
        scale = lax.rsqrt(jnp.mean(wide * wide, -N1, keepdims=True) + 1e-6)
        mean = jnp.mean(da * wide, -N1, keepdims=True)
        dw = da * scale - wide * (scale * scale * scale * mean)
        o_ref[...] = dh_ref[...] + dw.astype(BF16)

    def mm():
        da_ref[...] = dot_nt(dg_ref[...], wg_ref[...]) + dot_nt(du_ref[...], wu_ref[...])

    @pl.when(i == N0)
    def _():
        da_ref[...] = jnp.zeros_like(da_ref)

    @pl.when(i < steps)
    def _():
        epi()
        mm()

    @pl.when(i == steps)
    def _():
        epi()
        ring.finish(plan, steps + N1)
        ring.leave()
        for copy in copies:
            copy.wait()
        ss_out[...] = ss_in[...] + jnp.sum(ss[...])


def dx(layer, n, dg, du, wg, wu, h, dh, dw, gg, ss, gd, tb=256, spans=(), slack=0.0):
    t, ff = dg.shape
    d = dh.shape[N1]
    once = pl.Buffered(N1)
    steps = t // tb

    def cur(i):
        return (jnp.minimum(i, steps - N1), N0)

    def prv(i):
        return (jnp.maximum(i - N1, N0), N0)

    w_spec = pl.BlockSpec((None, d, ff), lambda i: (layer, N0, N0), pipeline_mode=once)
    anywhere = pl.BlockSpec(memory_space=pl.ANY)
    small = pl.BlockSpec((8, 128), lambda i: (N0, N0))
    wide = max(w for _, w in spans)
    cfg = (n, steps, spans, slack)
    return pl.pallas_call(
        functools.partial(dx_kernel, cfg),
        grid=(steps + N1,),
        in_specs=[
            pl.BlockSpec((tb, ff), cur),
            pl.BlockSpec((tb, ff), cur),
            w_spec,
            w_spec,
            pl.BlockSpec((tb, d), prv),
            pl.BlockSpec((tb, d), prv),
            anywhere,
            anywhere,
            small,
            anywhere,
        ],
        out_specs=[pl.BlockSpec((tb, d), prv), anywhere, anywhere, small, anywhere],
        out_shape=[
            jax.ShapeDtypeStruct((t, d), BF16),
            jax.ShapeDtypeStruct((len(spans), n - N1, N2, d // n, wide), BF16),
            jax.ShapeDtypeStruct(gg.shape, BF16),
            jax.ShapeDtypeStruct((8, 128), F32),
            jax.ShapeDtypeStruct((N2, EARLY_ROWS, d), BF16),
        ],
        scratch_shapes=[pltpu.VMEM((tb, d), F32)]
        + [pltpu.VMEM((N2, n - N1, N2, d // n, wide), BF16)] * N2
        + [pltpu.VMEM((8, wide), F32)]
        + ring_sems(n, len(spans))
        + [pltpu.SemaphoreType.DMA((N2,))] * N2,
        input_output_aliases={7: N2},
        compiler_params=pltpu.CompilerParams(
            vmem_limit_bytes=60 << 20, dimension_semantics=("arbitrary",), collective_id=3, has_side_effects=True
        ),
        cost_estimate=pl.CostEstimate(flops=4 * t * d * ff, bytes_accessed=4 * t * ff, transcendentals=N0),
        name=f"dx{layer}",
    )(dg, du, wg, wu, h, dh, dw, gg, ss, gd)


def place_near(n, own, left, right, after):
    layers, rows, cols = own.shape

    def body(where_ref, *refs):
        for which, ref in enumerate(refs[:3]):

            @pl.when(pl.program_id(N0) == which)
            def _():
                refs[-N1][...] = ref[...]

    some = 64
    block, per = (layers, some, cols), rows // some

    def at(device):
        return pl.BlockSpec(block, lambda k, r, where_ref: (N0, jnp.where(k < device, N0, jnp.where(k > device, per - N1, r)), N0))

    return pl.pallas_call(
        body,
        grid_spec=pltpu.PrefetchScalarGridSpec(
            num_scalar_prefetch=N1,
            grid=(3, per),
            in_specs=[at(N0), at(N1), at(N2)] + [pl.BlockSpec(memory_space=pl.ANY)] * len(after),
            out_specs=pl.BlockSpec(block, lambda k, r, where_ref: (N0, where_ref[k] * per + r, N0)),
        ),
        out_shape=jax.ShapeDtypeStruct((layers, n * rows, cols), own.dtype),
        compiler_params=pltpu.CompilerParams(vmem_limit_bytes=40 << 20, dimension_semantics=("arbitrary", "arbitrary")),
        cost_estimate=pl.CostEstimate(flops=N0, bytes_accessed=12 * layers * rows * cols, transcendentals=N0),
        name="place_near",
    )(whereabouts(n), own, left, right, *after)


def place_far(n, into, far, after):
    rows, cols = far[N0].shape

    def body(where_ref, far0_ref, far1_ref, into_ref, *refs):
        for which, ref in enumerate((far0_ref, far1_ref)):

            @pl.when(pl.program_id(N0) == which)
            def _():
                refs[-N1][...] = ref[...]

    whole = pl.BlockSpec((rows, cols), lambda k, where_ref: (N0, N0))
    anywhere = pl.BlockSpec(memory_space=pl.ANY)
    return pl.pallas_call(
        body,
        grid_spec=pltpu.PrefetchScalarGridSpec(
            num_scalar_prefetch=N1,
            grid=(N2,),
            in_specs=[whole, whole, anywhere, *[anywhere] * len(after)],
            out_specs=pl.BlockSpec((None, rows, cols), lambda k, where_ref: (k, where_ref[3], N0)),
        ),
        out_shape=jax.ShapeDtypeStruct(into.shape, into.dtype),
        input_output_aliases={3: N0},
        compiler_params=pltpu.CompilerParams(vmem_limit_bytes=40 << 20, dimension_semantics=("arbitrary",)),
        cost_estimate=pl.CostEstimate(flops=N0, bytes_accessed=8 * rows * cols, transcendentals=N0),
        name="place_far",
    )(whereabouts(n), *far, into, *after)


def step_kernel(factor_ref, w_ref, m_ref, v_ref, g0_ref, g1_ref, *refs):
    w_out, m_out, v_out = refs[-3:]
    for layer, g_ref in enumerate((g0_ref, g1_ref)):

        @pl.when(pl.program_id(N0) == layer)
        def _():

            @pl.loop(N0, w_ref.shape[N0] // 16)
            def _(r):
                at = pl.ds(pl.multiple_of(r * 16, 16), 16)
                g = g_ref[at, :].astype(F32) * factor_ref[N0, N0]
                w_out[at, :], m_out[at, :], v_out[at, :] = adamw(w_ref[at, :].astype(F32), m_ref[at, :], v_ref[at, :], g)


def own_step(n, factor, w, m, v, grads, which, after, rb):
    layers, rows, cols = m.shape
    per = rows // rb
    me = lax.axis_index("dp").reshape(N1)

    def body(me_ref, *refs):
        step_kernel(*refs)

    mine = pl.BlockSpec((None, rb, cols), lambda k, r, me_ref: (k, r, N0))

    def at(layer):
        def index(k, r, me_ref):
            r = jnp.where(k < layer, N0, jnp.where(k > layer, per - N1, r))
            return (r, N0) if which is None else (which, r, N0)

        return pl.BlockSpec((rb, cols) if which is None else (None, rb, cols), index)

    return pl.pallas_call(
        body,
        grid_spec=pltpu.PrefetchScalarGridSpec(
            num_scalar_prefetch=N1,
            grid=(layers, per),
            in_specs=[
                pl.BlockSpec(memory_space=pltpu.SMEM),
                pl.BlockSpec((None, rb, cols), lambda k, r, me_ref: (k, me_ref[N0] * per + r, N0)),
                mine,
                mine,
                at(N0),
                at(N1),
                *[pl.BlockSpec(memory_space=pl.ANY)] * len(after),
            ],
            out_specs=[mine] * 3,
        ),
        out_shape=[jax.ShapeDtypeStruct(m.shape, t) for t in (BF16, F32, F32)],
        compiler_params=pltpu.CompilerParams(vmem_limit_bytes=50 << 20, dimension_semantics=("arbitrary", "arbitrary")),
        cost_estimate=pl.CostEstimate(flops=20 * m.size, bytes_accessed=22 * m.size, transcendentals=m.size),
        name="own_step",
    )(me, factor, w, m, v, *grads, *after)


def ways(n):
    return [(i, (i + N1) % n) for i in range(n)], [(i, (i - N1) % n) for i in range(n)]


def neighbours(own, n):
    return [lax.ppermute(own, "dp", way) for way in ways(n)]


def far_parts(left, right, n):
    return [lax.ppermute(t, "dp", way) for t, way in zip((left, right), ways(n))]


def whereabouts(n):
    return (lax.axis_index("dp") + jnp.array([N0, n - N1, N1, N2], jnp.int32)) % n


def early_step(n, layer, factor, w, m, v, near, far, g, g_near, g_far, after):
    rows, cols = w.shape[N1:]
    count, per = EARLY_ROWS // ROWS, rows // n // ROWS

    def body(where_ref, factor_ref, om, ov, lmv, rmv, fm, fv, og, lg, rg, fg, w_ref, *refs):
        out_ref = refs[-N1]
        k, r = pl.program_id(N0), pl.program_id(N1)

        def step(m, v, g):
            @pl.loop(N0, ROWS // 16)
            def _(i):
                at = pl.ds(pl.multiple_of(i * 16, 16), 16)
                out_ref[at, :] = adamw(w_ref[at, :].astype(F32), m[at, :], v[at, :], g[at, :].astype(F32) * factor_ref[N0, N0])[N0]

        @pl.when(k == N0)
        def _():
            step(om, ov, og)

        @pl.when(k == N1)
        def _():
            step(lmv.at[N0], lmv.at[N1], lg)

        @pl.when(k == N2)
        def _():
            step(rmv.at[N0], rmv.at[N1], rg)

        @pl.when(k == 3)
        def _():
            step(fm, fv, fg)

    def at(device, shape, *lead):
        def index(k, r, where_ref):
            return (*lead, jnp.where(k < device, N0, jnp.where(k > device, count - N1, r)), N0)

        return pl.BlockSpec(shape, index)

    def to(k, r, where_ref):
        return (layer, where_ref[k] * per + r, N0)

    one = (ROWS, cols)
    specs = [at(N0, (None, *one), layer)] * N2 + [at(N1 + way, (None, N2, *one), way, N0) for way in (N0, N1)]
    specs += [at(3, (None, *one), kind) for kind in (N0, N1)]
    specs += [at(N0, one), at(N1, (None, *one), N0), at(N2, (None, *one), N1), at(3, one)]
    return pl.pallas_call(
        body,
        grid_spec=pltpu.PrefetchScalarGridSpec(
            num_scalar_prefetch=N1,
            grid=(n, count),
            in_specs=[pl.BlockSpec(memory_space=pltpu.SMEM), *specs, pl.BlockSpec((None, *one), to), *[pl.BlockSpec(memory_space=pl.ANY)] * len(after)],
            out_specs=pl.BlockSpec((None, *one), to),
        ),
        out_shape=jax.ShapeDtypeStruct(w.shape, w.dtype),
        compiler_params=pltpu.CompilerParams(vmem_limit_bytes=50 << 20, dimension_semantics=("arbitrary", "arbitrary")),
        cost_estimate=pl.CostEstimate(flops=N0, bytes_accessed=14 * n * EARLY_ROWS * cols, transcendentals=N0),
        name="early_step",
    )(whereabouts(n), factor, m, v, near, near, far, far, g, g_near, g_near, g_far, w, *after)


def place_rest(n, layer, into, parts, first, after):
    cols = parts[N0].shape[N1]
    per = into.shape[N1] // n // ROWS
    counts = [part.shape[N0] // ROWS for part in parts]
    whole = max(counts) if first == N0 else sum(counts)
    starts = [i * whole for i in range(len(parts))] if first == N0 else [N0, counts[N0]]

    def body(where_ref, *refs):
        i = pl.program_id(N0)
        for ref, start, count in zip(refs, starts, counts):

            @pl.when((i >= start) & (i < start + count))
            def _():
                refs[-N1][...] = ref[...]

    def at(start, count):
        return pl.BlockSpec((ROWS, cols), lambda i, where_ref: (jnp.clip(i - start, N0, count - N1), N0))

    def to(i, where_ref):
        r = lax.rem(i, whole)
        over = r >= per
        return (jnp.where(over, layer, N0), where_ref[first + i // whole] * per + jnp.where(over, r - per + EARLY_ROWS // ROWS, r), N0)

    anywhere = pl.BlockSpec(memory_space=pl.ANY)
    return pl.pallas_call(
        body,
        grid_spec=pltpu.PrefetchScalarGridSpec(
            num_scalar_prefetch=N1,
            grid=(sum(counts),),
            in_specs=[*map(at, starts, counts), anywhere, *[anywhere] * len(after)],
            out_specs=pl.BlockSpec((None, ROWS, cols), to),
        ),
        out_shape=jax.ShapeDtypeStruct(into.shape, into.dtype),
        input_output_aliases={N1 + len(parts): N0},
        compiler_params=pltpu.CompilerParams(vmem_limit_bytes=40 << 20, dimension_semantics=("arbitrary",)),
        cost_estimate=pl.CostEstimate(flops=N0, bytes_accessed=4 * sum(counts) * ROWS * cols, transcendentals=N0),
        name="place_rest",
    )(whereabouts(n), *parts, into, *after)


def adamw(w, m, v, g):
    m = 0.9 * m + 0.1 * g
    v = 0.95 * v + 0.05 * g * g
    step = m * lax.rsqrt(v + 1e-8) + 0.1 * w
    return (w - 0.02 * step).astype(BF16), m, v


def solution(mesh):
    n = mesh.shape["dp"]

    def of_a_device(x, dy, wg, wu, wd, *moments):
        x, dy = x[N0], dy[N0]
        m, v = moments[:3], moments[3:]
        ff = wg.shape[N2]
        a0, g0, u0, act0, h1, near = fwd(N0, n, x, wg, wu, wd, moving=[m[N2], v[N2]])
        a1, g1, u1, act1, far = fwd(N1, n, h1, wg, wu, moving=[near])
        mine = dwd(act1, dy, (), rb=400)
        dw1, _, _, gd1, gg1, ss, dg, du = bwd(N1, n, g1, u1, dy, wd, a1, mine, spans=spans_of(ff, 512, N0, 3), slack=2.0)
        dh, _, gg1, ss, g_near = dx(N1, n, dg, du, wg, wu, h1, dy, dw1, gg1, ss, gd1, spans=spans_of(ff, 512, 3, 5), slack=1.0)
        mine, _, gg1, ss, g_far = dwd_ring(n, act0, dh, dw1, gg1, ss, g_near, spans_of(ff, 512, 5))
        _, _, _, gd0, gg0, ss = bwd(N0, n, g0, u0, dh, wd, a0, mine, ss, spans=spans_of(ff, 256))
        count = sum(w.size for w in (wg, wu, wd))
        factor = jnp.minimum(1.0, 0.5 * lax.rsqrt(ss[N0, N0] / count + 1e-30))
        factor = factor.reshape(N1, N1)
        gate = own_step(n, factor, wg, m[N0], v[N0], (gg0, gg1), N0, (), 64)
        gate_near = neighbours(gate[N0], n)
        up = own_step(n, factor, wu, m[N1], v[N1], (gg0, gg1), N1, (gate[N0],), 64)
        up_near = neighbours(up[N0], n)
        down = own_step(n, factor, wd, m[N2], v[N2], (gd0, gd1), None, (up[N0],), 160)
        rest = jnp.concatenate([down[N0][N0], down[N0][N1, EARLY_ROWS:]])
        rest_near = neighbours(rest, n)
        early = early_step(n, N1, factor, wd, m[N2], v[N2], near, far, gd1, g_near, g_far, (rest,))
        gate_far = far_parts(gate_near[N0][N0], gate_near[N1][N1], n)
        cut = ROWS * (rest.shape[N0] // ROWS // N2)
        rest_far = far_parts(rest_near[N0][:cut], rest_near[N1][cut:], n)
        up_far = far_parts(up_near[N0][N0], up_near[N1][N1], n)
        new_gate = place_far(n, place_near(n, gate[N0], *gate_near, (early,)), gate_far, ())
        new_up = place_near(n, up[N0], *up_near, (new_gate,))
        new_down = place_rest(n, N1, early, [rest, *rest_near], N0, (new_up,))
        new_up = place_far(n, new_up, up_far, (new_down,))
        new_down = place_rest(n, N1, new_down, rest_far, 3, (new_up,))
        whole = (new_gate, new_up, new_down)
        new = (gate, up, down)
        return tuple(whole) + tuple(one[N1] for one in new) + tuple(one[N2] for one in new)

    seq = P(("rep", "dp"))
    whole, rows = P(), P(None, "dp")
    return jax.shard_map(
        of_a_device,
        mesh=mesh,
        in_specs=(seq, seq) + (whole,) * 3 + (rows,) * 6,
        out_specs=(P("rep"),) * 3 + (P("rep", "dp"),) * 6,
        check_vma=False,
    )
```
